32 devices in a mesh: dp: 16 (over z, y, x), tensor: 2 (over core).
Axes of the slice: x: 2, y: 2, z: 4, core: 2. Of those that a mesh axis runs over, the one named last changes fastest.
Arguments:
- inputs: bfloat16 [16384, 512], P('dp'), may hold values from -6 to 6
- w_qkv: bfloat16 [3, 512, 512], P(None, None, 'tensor'), may hold values from -0.25 to 0.25
- b_qv: float32 [2, 512], P(None, 'tensor'), may hold values from -1.2 to 1.2
- w_out: bfloat16 [512, 512], P('tensor'), may hold values from -3 to 3
- b_out: float32 [512], replicated, may hold values from -3 to 3
- norm1_gain: float32 [512], replicated, may hold values from 0.1 to 1.9
- norm1_shift: float32 [512], replicated, may hold values from -3 to 3
- w_in: bfloat16 [512, 1024], P(None, 'tensor'), may hold values from -0.25 to 0.25
- b_in: float32 [1024], P('tensor'), may hold values from -3 to 3
- w_down: bfloat16 [1024, 512], P('tensor'), may hold values from -0.25 to 0.25
- b_down: float32 [512], replicated, may hold values from -3 to 3
- norm2_gain: float32 [512], replicated, may hold values from 0.1 to 1.9
- norm2_shift: float32 [512], replicated, may hold values from -3 to 3
- segment_ids: int32 [16, 1024], P('dp'), may hold values from 0 to 9, as said below
- d_out: bfloat16 [16384, 512], P(('dp', 'tensor')), may hold values from -6 to 6
Outputs:
- output: bfloat16 [16384, 512], P(('dp', 'tensor'))
- d_inputs: bfloat16 [16384, 512], P(('dp', 'tensor'))
- grad_w_qkv: float32 [3, 512, 512], P(None, None, 'tensor')
- grad_b_qv: float32 [2, 512], P(None, 'tensor')
- grad_w_out: float32 [512, 512], P('tensor')
- grad_b_out: float32 [512], replicated
- grad_norm1_gain: float32 [512], replicated
- grad_norm1_shift: float32 [512], replicated
- grad_w_in: float32 [512, 1024], P(None, 'tensor')
- grad_b_in: float32 [1024], P('tensor')
- grad_w_down: float32 [1024, 512], P('tensor')
- grad_b_down: float32 [512], replicated
- grad_norm2_gain: float32 [512], replicated
- grad_norm2_shift: float32 [512], replicated
The draws below stay inside these ranges and needn't reach their ends.
Inputs may be any that keep to these rules, and one draw needn't show every extreme that they name: `segment_ids`: along a row the ids never fall until the trailing padding; datasets carry ids 1 to 9, padding carries 0 and stands only at a row's end; row 0 has no padding.
All inputs are finite; a program needn't handle non-finite values.
Results may differ from the reference program's by a relative error of at most 0.02.
Values may be sent and summed in bfloat16 or wider, within the bound.
A program may use at most 64 MiB of HBM per device.

```python
import jax
import jax.numpy as jnp
from jax import lax

D = 512
HEADS = 4
HD = 128
FF = 1024
LEN = 1024
SETS = 8
QBLK = 512
BATCH = 16
TOKENS = 16384


def draw_segment_ids(key, part):
    start_key, pad_key = jax.random.split(key)
    starts = jax.random.randint(start_key, (BATCH, SETS), 1, LEN)
    positions = jnp.arange(LEN, dtype=jnp.int32)
    labels = 1 + jnp.sum((positions[None, :, None] >= starts[:, None, :]).astype(jnp.int32), -1)
    padding = jax.random.randint(pad_key, (BATCH, 1), 0, LEN // 4 + 1)
    padding = padding * (jnp.arange(BATCH)[:, None] != 0).astype(jnp.int32)
    return jnp.where(positions[None, :] >= LEN - padding, 0, labels).astype(jnp.int32)


def block_scale(stream_key, shape, cuts, smallest, top_value):
    factor_of = 1.0
    for dim, blocks in cuts:
        heights = jax.random.uniform(jax.random.fold_in(jax.random.fold_in(stream_key, 6), dim), (blocks,), jnp.float32, smallest / len(cuts), top_value / len(cuts))
        factor_of = factor_of * jnp.repeat(jnp.exp(heights), shape[dim] // blocks).reshape((-1,) + (1,) * (len(shape) - 1 - dim))
    return factor_of


def normal_values(own_key, extent, scale, limit, cuts=(), held_as=jnp.bfloat16):
    entries = scale * jax.random.normal(own_key, extent, jnp.float32)
    if cuts:
        entries = entries * block_scale(own_key, extent, cuts, -0.22, 0.18)
    return jnp.clip(entries, -limit, limit).astype(held_as)


def setup_inputs(seed: int = 0) -> dict:
    seeds = jax.random.split(jax.random.key(seed), 16)
    inputs = normal_values(seeds[0], (TOKENS, D), 1.0, 6.0, ((0, 16),))
    w_qkv = normal_values(seeds[1], (3, D, D), D ** -0.5, 0.25, ((2, 2),))
    b_qv = normal_values(seeds[2], (2, D), 0.2, 1.2, ((1, 2),), jnp.float32)
    w_out = normal_values(seeds[3], (D, D), (max(1, D * SETS // LEN)) ** -0.5, 3.0, ((0, 2),))
    b_out = normal_values(seeds[4], (D,), 0.5, 3.0, (), jnp.float32)
    norm1_gain = jnp.clip(1.0 + 0.18 * jax.random.normal(seeds[5], (D,), jnp.float32), 0.1, 1.9)
    norm1_shift = normal_values(seeds[6], (D,), 0.5, 3.0, (), jnp.float32)
    w_in = normal_values(seeds[7], (D, FF), D ** -0.5, 0.25, ((1, 2),))
    b_in = normal_values(seeds[8], (FF,), 0.5, 3.0, ((0, 2),), jnp.float32)
    w_down = normal_values(seeds[9], (FF, D), (FF // 2) ** -0.5, 0.25, ((0, 2),))
    b_down = normal_values(seeds[10], (D,), 0.5, 3.0, (), jnp.float32)
    norm2_gain = jnp.clip(1.0 + 0.18 * jax.random.normal(seeds[11], (D,), jnp.float32), 0.1, 1.9)
    norm2_shift = normal_values(seeds[12], (D,), 0.5, 3.0, (), jnp.float32)
    segment_ids = draw_segment_ids(jax.random.fold_in(seeds[15], 71), 0)
    d_out = normal_values(seeds[14], (TOKENS, D), 1.0, 6.0, ((0, 32),))
    return dict(inputs=inputs, w_qkv=w_qkv, b_qv=b_qv, w_out=w_out, b_out=b_out, norm1_gain=norm1_gain, norm1_shift=norm1_shift, w_in=w_in, b_in=b_in, w_down=w_down, b_down=b_down, norm2_gain=norm2_gain, norm2_shift=norm2_shift, segment_ids=segment_ids, d_out=d_out)


@jax.custom_vjp
def low(v):
    return lax.optimization_barrier(v.astype(jnp.bfloat16)).astype(jnp.float32)

@jax.custom_vjp
def low_back(v):
    return v

def low_keep(v):
    return (low(v), None)

def low_pass(kept, grad):
    return (grad,)

def back_keep(v):
    return (v, None)

def back_low(kept, grad):
    return (low(grad),)
low.defvjp(low_keep, low_pass)
low_back.defvjp(back_keep, back_low)
NORM_EPSILON = 1e-05
MASKED_SCORE = -1e+30
FULL_PRECISION = lax.Precision.HIGHEST

def both_ways(values):
    return low(low_back(values))

def layer_norm(values, norm_gain, norm_shift):
    average = lax.optimization_barrier(jnp.mean(values, -1, keepdims=True))
    centred = values - average
    spread = lax.optimization_barrier(jnp.mean(centred * centred, -1, keepdims=True))
    return centred * lax.rsqrt(spread + NORM_EPSILON) * norm_gain + norm_shift

def attend_block(query_blk, seg_blk, key_rows, values, segments):
    products = jnp.einsum('qhd,khd->hqk', query_blk, key_rows, precision=FULL_PRECISION)
    scores = low_back(products * HD ** (-0.5))
    matching = seg_blk[:, None] == segments[None, :]
    scores = jnp.where(matching[None], scores, MASKED_SCORE)
    attn_probs = jax.nn.softmax(scores, axis=-1)
    mixture = jnp.einsum('hqk,khd->qhd', low(attn_probs), values, precision=FULL_PRECISION)
    return mixture.reshape(mixture.shape[0], -1)

def sequence_forward(inputs_seq, segments, params):
    w_qkv, b_qv, w_out, b_out, norm1_gain, norm1_shift, w_in, b_in, w_down, b_down, norm2_gain, norm2_shift = params
    projected = jnp.einsum('td,cde->cte', inputs_seq, w_qkv, precision=FULL_PRECISION)
    queries = both_ways(projected[0] + b_qv[0]).reshape(LEN, HEADS, HD)
    key_rows = both_ways(projected[1]).reshape(LEN, HEADS, HD)
    values = both_ways(projected[2] + b_qv[1]).reshape(LEN, HEADS, HD)
    block_count = LEN // QBLK
    query_blocks = queries.reshape(block_count, QBLK, HEADS, HD)
    seg_blocks = segments.reshape(block_count, QBLK)

    def one_block(pieces):
        return attend_block(pieces[0], pieces[1], key_rows, values, segments)
    mixture = lax.map(jax.checkpoint(one_block), (query_blocks, seg_blocks)).reshape(LEN, D)
    mixture = both_ways(mixture)
    attn_out = low_back(jnp.dot(mixture, w_out, precision=FULL_PRECISION) + b_out)
    hidden = layer_norm(inputs_seq + attn_out, norm1_gain, norm1_shift)
    up_proj = low_back(jnp.dot(low(hidden), w_in, precision=FULL_PRECISION) + b_in)
    activated = low(jax.nn.gelu(up_proj, approximate=False))
    down_proj = low_back(jnp.dot(activated, w_down, precision=FULL_PRECISION) + b_down)
    row_mask = (segments != 0).astype(jnp.float32)[:, None]
    return layer_norm(hidden + down_proj, norm2_gain, norm2_shift) * row_mask

def reference(inputs, w_qkv, b_qv, w_out, b_out, norm1_gain, norm1_shift, w_in, b_in, w_down, b_down, norm2_gain, norm2_shift, segment_ids, d_out):
    params = tuple((weight.astype(jnp.float32) for weight in (w_qkv, b_qv, w_out, b_out, norm1_gain, norm1_shift, w_in, b_in, w_down, b_down, norm2_gain, norm2_shift)))
    group_size = min(BATCH, max(1, 4096 // LEN))
    group_count = BATCH // group_size
    input_groups = inputs.astype(jnp.float32).reshape(group_count, group_size, LEN, D)
    seg_groups = segment_ids.reshape(group_count, group_size, LEN)
    cot_groups = d_out.astype(jnp.float32).reshape(group_count, group_size, LEN, D)

    def one_group(totals, pieces):
        group_inputs, group_segments, group_cots = pieces

        def forward(inputs_in, params_in):
            return jax.vmap(sequence_forward, in_axes=(0, 0, None))(inputs_in, group_segments, params_in)
        result, pullback = jax.vjp(forward, group_inputs, params)
        grad_inputs, grad_params = pullback(group_cots)
        totals = jax.tree.map(lambda total_now, grad_now: total_now + grad_now, totals, grad_params)
        return (totals, (result.astype(jnp.bfloat16), grad_inputs.astype(jnp.bfloat16)))
    zero_grads = tuple((jnp.zeros_like(weight) for weight in params))
    totals, (results, grad_rows) = lax.scan(one_group, zero_grads, (input_groups, seg_groups, cot_groups))
    return (results.reshape(TOKENS, D), grad_rows.reshape(TOKENS, D), totals[0], totals[1], totals[2], totals[3], totals[4], totals[5], totals[6], totals[7], totals[8], totals[9], totals[10], totals[11])
```

```python
import jax
import jax.numpy as jnp
from jax import lax
from jax.experimental import pallas as pl
from jax.experimental.pallas import tpu as pltpu
from jax.sharding import PartitionSpec as P

HD = 128
NORM_EPSILON = 1e-05
MASKED_SCORE = -1e30
LOG2E = 1.4426950408889634
F32 = jnp.float32
BF16 = jnp.bfloat16
MESH = pl.DeviceIdType.MESH


def nn(a, b):
    return lax.dot_general(a, b, (((1,), (0,)), ((), ())), preferred_element_type=F32)


def nt(a, b):
    return lax.dot_general(a, b, (((1,), (1,)), ((), ())), preferred_element_type=F32)


def tn(a, b):
    return lax.dot_general(a, b, (((0,), (0,)), ((), ())), preferred_element_type=F32)


def torus_sizes(chips):
    side = 1
    for k in range(1, chips + 1):
        if chips % (k * k) == 0 and chips // (k * k) >= k:
            side = k
    return side, side, chips // (side * side)


class Semaphores:
    def __init__(self):
        self.count = 0

    def take(self, n=1):
        first = self.count
        self.count += n
        return first


class Stage:
    def __init__(self, size, place, peer, sems, send_sem, recv_sem):
        self.size, self.place, self.peer = size, place, peer
        self.first = sems.take(size - 1)
        self.send_sem, self.recv_sem = send_sem, recv_sem

    def to(self, j):
        return lax.rem(self.place + j, self.size)

    def copy(self, j, src, dst):
        slot = self.first + j - 1
        return pltpu.make_async_remote_copy(
            src_ref=src,
            dst_ref=dst,
            send_sem=self.send_sem.at[slot],
            recv_sem=self.recv_sem.at[slot],
            device_id=self.peer(self.to(j)),
            device_id_type=MESH,
        )


def blk(start, size, align=None):
    return pl.ds(pl.multiple_of(start, align or size), size)


class Reduction:
    def __init__(self, rows, axes, sems, send_sem, recv_sem):
        (n1, m1, peer1), (n2, m2, peer2), (n3, m3, peer3) = axes
        self.rows = rows
        self.p1, self.p2 = rows // n1, rows // (n1 * n2)
        self.split_z = (self.p2 // n3) % 16 == 0 and self.p2 % n3 == 0
        self.p3 = self.p2 // n3 if self.split_z else self.p2
        self.n1, self.n2, self.n3 = n1, n2, n3
        self.m1, self.m2, self.m3 = m1, m2, m3
        make = lambda n, m, peer: Stage(n, m, peer, sems, send_sem, recv_sem)
        self.s1, self.s2, self.s3 = make(n1, m1, peer1), make(n2, m2, peer2), make(n3, m3, peer3)
        self.g1, self.g2 = make(n1, m1, peer1), make(n2, m2, peer2)
        self.g3 = make(n3, m3, peer3) if self.split_z else None

    @staticmethod
    def scratch(rows, cols, sizes):
        n1, n2, n3 = sizes
        p1, p2 = rows // n1, rows // (n1 * n2)
        split_z = (p2 // n3) % 16 == 0 and p2 % n3 == 0
        p3 = p2 // n3 if split_z else p2
        return [
            pltpu.VMEM((n1 - 1, p1, cols), BF16),
            pltpu.VMEM((p1, cols), BF16),
            pltpu.VMEM((n2 - 1, p2, cols), BF16),
            pltpu.VMEM((p2, cols), BF16),
            pltpu.VMEM((n3 - 1, p3, cols), BF16),
        ]

    def bind(self, grad, scratch, out):
        self.grad, self.out = grad, out
        self.r1, self.t1, self.r2, self.t2, self.r3 = scratch
        self.off1 = pl.multiple_of(self.m1 * self.p1, self.p1)
        self.off2 = pl.multiple_of(self.off1 + self.m2 * self.p2, self.p2)
        self.off3 = self.off2
        if self.split_z:
            self.off3 = pl.multiple_of(self.off2 + self.m3 * self.p3, self.p3)

    def sends(self, name):
        if name == "s1":
            return [self.s1.copy(j, self.grad.at[blk(self.s1.to(j) * self.p1, self.p1)], self.r1.at[j - 1]) for j in range(1, self.n1)]
        if name == "s2":
            return [self.s2.copy(j, self.t1.at[blk(self.s2.to(j) * self.p2, self.p2)], self.r2.at[j - 1]) for j in range(1, self.n2)]
        if name == "s3":
            if self.split_z:
                return [self.s3.copy(j, self.t2.at[blk(self.s3.to(j) * self.p3, self.p3)], self.r3.at[j - 1]) for j in range(1, self.n3)]
            return [self.s3.copy(j, self.t2, self.r3.at[j - 1]) for j in range(1, self.n3)]
        if name == "g3":
            if not self.split_z:
                return []
            piece = self.out.at[pl.ds(self.off3, self.p3)]
            return [self.g3.copy(j, piece, piece) for j in range(1, self.n3)]
        if name == "g2":
            piece = self.out.at[pl.ds(self.off2, self.p2)]
            return [self.g2.copy(j, piece, piece) for j in range(1, self.n2)]
        piece = self.out.at[pl.ds(self.off1, self.p1)]
        return [self.g1.copy(j, piece, piece) for j in range(1, self.n1)]

    def landed(self, name):
        if name not in ("g1", "g2", "g3"):
            return self.sends(name)
        if name == "g3" and not self.split_z:
            return []
        stage, base, size, n = {
            "g3": (self.g3, self.off2, self.p3, self.n3),
            "g2": (self.g2, self.off1, self.p2, self.n2),
            "g1": (self.g1, 0, self.p1, self.n1),
        }[name]
        found = []
        for j in range(1, n):
            sender = lax.rem(stage.place + n - j, n)
            piece = self.out.at[pl.ds(pl.multiple_of(base + sender * size, size), size)]
            found.append(stage.copy(j, piece, piece))
        return found

    def start(self, name):
        for c in self.sends(name):
            c.start()

    def arrive(self, name):
        for c in self.landed(name):
            c.wait_recv()

    def drain(self):
        for name in ("s1", "s2", "s3", "g3", "g2", "g1"):
            for c in self.sends(name):
                c.wait_send()

    def step(self, number):
        if number == 0:
            self.start("s1")
        elif number == 1:
            self.arrive("s1")
            total = self.grad[blk(self.m1 * self.p1, self.p1), :].astype(F32)
            for j in range(self.n1 - 1):
                total = total + self.r1[j].astype(F32)
            self.t1[...] = total.astype(BF16)
            self.start("s2")
        elif number == 2:
            self.arrive("s2")
            total = self.t1[blk(self.m2 * self.p2, self.p2), :].astype(F32)
            for j in range(self.n2 - 1):
                total = total + self.r2[j].astype(F32)
            self.t2[...] = total.astype(BF16)
            self.start("s3")
        elif number == 3:
            self.arrive("s3")
            if self.split_z:
                total = self.t2[blk(self.m3 * self.p3, self.p3), :].astype(F32)
            else:
                total = self.t2[...].astype(F32)
            for j in range(self.n3 - 1):
                total = total + self.r3[j].astype(F32)
            self.out[pl.ds(self.off3, self.p3), :] = total.astype(BF16)
            self.start("g3")
        elif number == 4:
            self.arrive("g3")
            self.start("g2")
        elif number == 5:
            self.arrive("g2")
            self.start("g1")
        else:
            self.arrive("g1")


def make_kernel(sizes, length, width, hidden_units):
    nx, ny, nz = sizes
    half = length // 2
    qb = 256
    fh = hidden_units // 2
    heads = 2
    hw = heads * HD
    kcat = 3 * HD
    score_c = HD ** (-0.5) * LOG2E
    key_rows = 512

    grads = (("a", fh, width), ("b", width, fh), ("c", hw, width), ("d0", width, kcat), ("d1", width, kcat))

    scratch = dict(
        xt=pltpu.VMEM((width, length), BF16),
        q=pltpu.VMEM((heads, length, HD), BF16),
        k=pltpu.VMEM((heads, length, HD), BF16),
        v=pltpu.VMEM((heads, length, HD), BF16),
        kt=pltpu.VMEM((heads, HD, length), BF16),
        vt=pltpu.VMEM((heads, HD, length), BF16),
        segf=pltpu.VMEM((1, length), F32),
        kb=pltpu.VMEM((length, qb), F32),
        lse=pltpu.VMEM((heads, 1, length), F32),
        mix=pltpu.VMEM((heads, length, HD), BF16),
        mo=pltpu.VMEM((heads, half, HD), BF16),
        wout_o=pltpu.VMEM((hw, width), BF16),
        win_o=pltpu.VMEM((width, fh), BF16),
        wdown_o=pltpu.VMEM((fh, width), BF16),
        bin_o=pltpu.VMEM((1, fh), F32),
        hid=pltpu.VMEM((half, width), BF16),
        act=pltpu.VMEM((2, half, fh), BF16),
        gp=pltpu.VMEM((2, qb, fh), F32),
        ddown=pltpu.VMEM((half, width), BF16),
        dup=pltpu.VMEM((2, half, fh), BF16),
        dattn=pltpu.VMEM((half, width), BF16),
        dpre=pltpu.VMEM((half, width), F32),
        dmix=pltpu.VMEM((heads, length, HD), BF16),
        dmo=pltpu.VMEM((heads, half, HD), BF16),
        dkacc=pltpu.VMEM((heads, length, HD), F32),
        dvacc=pltpu.VMEM((heads, length, HD), F32),
        dcat=pltpu.VMEM((heads, length, kcat), BF16),
        dxs=pltpu.VMEM((half, width), BF16),
        dxr=pltpu.VMEM((half, width), BF16),
        sm=pltpu.VMEM((16, width), F32),
        smt=pltpu.VMEM((16, width), F32),
        sm0=pltpu.VMEM((16, width), F32),
        sm1=pltpu.VMEM((16, width), F32),
        sm2=pltpu.VMEM((16, width), F32),
        smr1=pltpu.VMEM((nx - 1, 16, width), F32),
        smr2=pltpu.VMEM((ny - 1, 16, width), F32),
        smr3=pltpu.VMEM((nz - 1, 16, width), F32),
    )
    for name, rows, cols in grads:
        scratch["g_" + name] = pltpu.VMEM((rows, cols), BF16)
        if name in "abc":
            scratch["gs_" + name] = pltpu.VMEM((rows, cols), BF16)
            scratch["gr_" + name] = pltpu.VMEM((rows, cols), BF16)
        for i, spec in enumerate(Reduction.scratch(rows, cols, sizes)):
            scratch[f"red_{name}_{i}"] = spec

    names = list(scratch)
    n_sems = 256

    def kernel(x, wqkv, bqv, wout, bout, n1g, n1s, win, bin_, wdown, bdown, n2g, n2s, seg, dout, *rest):
        out_o, din_o, ga_o, gb_o, gc_o, gd0_o, gd1_o, small_o = rest[:8]
        refs = dict(zip(names, rest[8 : 8 + len(names)]))
        send_sem, recv_sem = rest[8 + len(names) :]
        s = type("Scratch", (), refs)
        sems = Semaphores()

        dp = lax.axis_index("dp")
        t = lax.axis_index("tensor")
        other = 1 - t
        xi = lax.rem(dp, nx)
        yi = lax.rem(lax.div(dp, nx), ny)
        zi = lax.div(dp, nx * ny)
        m1 = xi + t * (yi - xi)
        m2 = yi + t * (xi - yi)
        stride1 = 1 + t * (nx - 1)
        stride2 = nx + t * (1 - nx)
        peer1 = lambda c: (dp + (c - m1) * stride1, t)
        peer2 = lambda c: (dp + (c - m2) * stride2, t)
        peer3 = lambda c: (dp + (c - zi) * (nx * ny), t)
        axes = ((nx, m1, peer1), (ny, m2, peer2), (nz, zi, peer3))

        barrier = pltpu.get_barrier_semaphore()
        pl.semaphore_signal(barrier, inc=1, device_id=(dp, other), device_id_type=MESH)
        for n, m, peer in axes:
            for j in range(1, n):
                pl.semaphore_signal(barrier, inc=1, device_id=peer(lax.rem(m + j, n)), device_id_type=MESH)
        pl.semaphore_wait(barrier, 1 + (nx - 1) + (ny - 1) + (nz - 1))

        def across(src, dst, slot=None):
            slot = sems.take() if slot is None else slot
            return pltpu.make_async_remote_copy(
                src_ref=src, dst_ref=dst, send_sem=send_sem.at[slot], recv_sem=recv_sem.at[slot],
                device_id=(dp, other), device_id_type=MESH,
            )

        my0 = pl.multiple_of(t * half, half)
        ot0 = pl.multiple_of(other * half, half)
        all_copies = []

        def launch(*copies):
            for c in copies:
                c.start()
                all_copies.append(c)

        weights = [
            across(wout, s.wout_o),
            across(win, s.win_o),
            across(wdown, s.wdown_o),
            across(bin_, s.bin_o),
        ]
        launch(*weights)

        mix_out = [across(s.mix.at[h, pl.ds(ot0, half)], s.mo.at[h]) for h in range(heads)]
        dmix_slots = [sems.take() for _ in range(heads)]
        dmix_out = [across(s.dmo.at[h], s.dmix.at[h, pl.ds(my0, half)], dmix_slots[h]) for h in range(heads)]
        dmix_in = [across(s.dmo.at[h], s.dmix.at[h, pl.ds(ot0, half)], dmix_slots[h]) for h in range(heads)]
        part = {name: across(refs["gs_" + name], refs["gr_" + name]) for name in "abc"}
        dx_out = across(s.dxs, s.dxr)
        small_t = across(s.sm, s.smt)
        red = {}
        outs = dict(a=ga_o, b=gb_o, c=gc_o, d0=gd0_o, d1=gd1_o)
        for name, rows, cols in grads:
            red[name] = Reduction(rows, axes, sems, send_sem, recv_sem)
            red[name].bind(refs["g_" + name], [refs[f"red_{name}_{i}"] for i in range(5)], outs[name])
        small_stages = [Stage(n, m, peer, sems, send_sem, recv_sem) for n, m, peer in axes]
        small_bufs = [(s.sm0, s.smr1), (s.sm1, s.smr2), (s.sm2, s.smr3)]

        def small_copies(i):
            src, dst = small_bufs[i]
            return [small_stages[i].copy(j, src, dst.at[j - 1]) for j in range(1, axes[i][0])]

        assert sems.count <= n_sems

        segf = seg[...].astype(F32)
        s.segf[...] = segf
        for b in range(length // 128):
            rows = jnp.broadcast_to(s.segf[:, b * 128 : (b + 1) * 128], (128, 128)).T
            for c in range(qb // 128):
                s.kb[b * 128 : (b + 1) * 128, c * 128 : (c + 1) * 128] = rows

        def project(i, _):
            rows = blk(i * qb, qb)
            xb = x[rows, :]
            s.xt[:, rows] = xb.T
            qv = nn(xb, wqkv[0]) + bqv[0:1, :]
            kv = nn(xb, wqkv[1])
            vv = nn(xb, wqkv[2]) + bqv[1:2, :]
            ql, kl, vl = qv.astype(BF16), kv.astype(BF16), vv.astype(BF16)
            for h in range(heads):
                cols = slice(h * HD, (h + 1) * HD)
                s.q[h, rows, :] = ql[:, cols]
                s.k[h, rows, :] = kl[:, cols]
                s.v[h, rows, :] = vl[:, cols]
                s.kt[h, :, rows] = kl[:, cols].T
                s.vt[h, :, rows] = vl[:, cols].T
            return 0

        lax.fori_loop(0, length // qb, project, 0)

        def block_scores(h, rows):
            products = nt(s.k[h], s.q[h, rows, :]) * score_c
            return jnp.where(s.kb[...] == s.segf[:, rows], products, MASKED_SCORE)

        blocks = length // qb

        def attend(i, _):
            h = lax.rem(i, heads)
            qi = lax.rem(other * (blocks // 2) + lax.div(i, heads), blocks)
            rows = blk(qi * qb, qb)
            scores = block_scores(h, rows)
            top = jnp.max(scores, 0, keepdims=True)
            weights_t = jnp.exp2(scores - top)
            total = jnp.sum(weights_t, 0, keepdims=True)
            mixed = nn(s.vt[h], weights_t.astype(BF16)) * (1.0 / total)
            s.mix[h, rows, :] = mixed.T.astype(BF16)
            s.lse[h, :, rows] = top + jnp.log2(total)
            return 0

        n_att = heads * blocks
        lax.fori_loop(0, n_att // 2, attend, 0)
        launch(*mix_out)
        lax.fori_loop(n_att // 2, n_att, attend, 0)
        for c in weights + mix_out:
            c.wait_recv()

        s.sm[...] = jnp.zeros_like(s.sm)

        def add_small(row, value):
            s.sm[row : row + 1, :] += value

        def row_sum(value):
            return jnp.sum(value, 0, keepdims=True)

        def norm(v):
            average = jnp.mean(v, -1, keepdims=True)
            centred = v - average
            rs = lax.rsqrt(jnp.mean(centred * centred, -1, keepdims=True) + NORM_EPSILON)
            return centred * rs, rs

        def norm_back(e, n, rs):
            return (e - jnp.mean(e, -1, keepdims=True) - n * jnp.mean(e * n, -1, keepdims=True)) * rs

        halves = ((win, bin_, wdown, wout), (s.win_o, s.bin_o, s.wdown_o, s.wout_o))

        def middle(r, _):
            here = blk(r * qb, qb)
            whole = pl.ds(pl.multiple_of(my0 + r * qb, qb), qb)
            mine = jnp.concatenate([s.mix[h, whole, :] for h in range(heads)], 1)
            theirs = jnp.concatenate([s.mo[h, here, :] for h in range(heads)], 1)
            pre1 = x[whole, :].astype(F32) + (nn(mine, wout[...]) + nn(theirs, s.wout_o[...]) + bout[...])
            n1, rs1 = norm(pre1)
            hidden = n1 * n1g[...] + n1s[...]
            low = hidden.astype(BF16)
            s.hid[here, :] = low
            for f, (w_in, b_in, _, _) in enumerate(halves):
                up = nn(low, w_in[...]) + b_in[...]
                cdf = 0.5 * (1.0 + lax.erf(up * (0.5**0.5)))
                s.act[f, here, :] = (up * cdf).astype(BF16)
                s.gp[f] = cdf + up * (jnp.exp2(up * up * (-0.5 * LOG2E)) * 0.3989422804014327)
            down = nn(s.act[0, here, :], wdown[...]) + nn(s.act[1, here, :], s.wdown_o[...]) + bdown[...]
            n2, rs2 = norm(hidden + down)
            row_mask = (s.kb[whole, 0:1] != 0.0).astype(F32)
            out_o[here, :] = ((n2 * n2g[...] + n2s[...]) * row_mask).astype(BF16)
            cot = dout[here, :].astype(F32) * row_mask
            add_small(0, row_sum(cot))
            add_small(1, row_sum(cot * n2))
            d_resid = norm_back(cot * n2g[...], n2, rs2)
            d_down = d_resid.astype(BF16)
            s.ddown[here, :] = d_down
            add_small(2, row_sum(d_down.astype(F32)))
            d_hidden = d_resid
            for f, (w_in, _, w_down, _) in enumerate(halves):
                d_up = (nt(d_down, w_down[...]) * s.gp[f]).astype(BF16)
                s.dup[f, here, :] = d_up
                add_small(3 + f, row_sum(d_up.astype(F32)))
                d_hidden = d_hidden + nt(d_up, w_in[...])
            add_small(5, row_sum(d_hidden))
            add_small(6, row_sum(d_hidden * n1))
            d_pre = norm_back(d_hidden * n1g[...], n1, rs1)
            s.dpre[here, :] = d_pre
            d_attn = d_pre.astype(BF16)
            s.dattn[here, :] = d_attn
            add_small(7, row_sum(d_attn.astype(F32)))
            dm = nt(d_attn, wout[...]).astype(BF16)
            do = nt(d_attn, s.wout_o[...]).astype(BF16)
            for h in range(heads):
                s.dmix[h, whole, :] = dm[:, h * HD : (h + 1) * HD]
                s.dmo[h, here, :] = do[:, h * HD : (h + 1) * HD]
            return 0

        lax.fori_loop(0, half // qb, middle, 0)
        launch(*dmix_out)

        def grad_block(dst, lhs, rhs):
            n = lhs.shape[1]

            def body(i, _):
                cols = blk(i * qb, qb)
                dst[cols, :] = tn(lhs[:, cols], rhs[...]).astype(BF16)
                return 0

            lax.fori_loop(0, n // qb, body, 0)

        grad_block(s.gs_a, s.act.at[1], s.ddown)
        launch(part["a"])
        grad_block(s.g_a, s.act.at[0], s.ddown)
        grad_block(s.gs_b, s.hid, s.dup.at[1])
        launch(part["b"])

        def join(name):
            part[name].wait_recv()
            mine, theirs = refs["g_" + name], refs["gr_" + name]
            mine[...] = (mine[...].astype(F32) + theirs[...].astype(F32)).astype(BF16)
            red[name].step(0)

        join("a")
        grad_block(s.g_b, s.hid, s.dup.at[0])
        theirs = jnp.concatenate([s.mo[h] for h in range(heads)], 1)
        s.gs_c[...] = tn(theirs, s.dattn[...]).astype(BF16)
        launch(part["c"])
        join("b")
        mine = jnp.concatenate([s.mix[h, pl.ds(my0, half), :] for h in range(heads)], 1)
        s.g_c[...] = tn(mine, s.dattn[...]).astype(BF16)
        join("c")

        s.dkacc[...] = jnp.zeros_like(s.dkacc)
        s.dvacc[...] = jnp.zeros_like(s.dvacc)
        for c in dmix_in:
            c.wait_recv()

        def finish_head(h):
            dk = (s.dkacc[h] * (HD ** (-0.5))).astype(BF16)
            dv = s.dvacc[h].astype(BF16)
            s.dcat[h, :, HD : 2 * HD] = dk
            s.dcat[h, :, 2 * HD :] = dv
            s.sm[8:9, h * HD : (h + 1) * HD] = row_sum(s.dcat[h, :, 0:HD].astype(F32))
            s.sm[8:9, hw + h * HD : hw + (h + 1) * HD] = row_sum(dv.astype(F32))
            dst = s.g_d0 if h == 0 else s.g_d1

            def body(i, _):
                rows = blk(i * 128, 128)
                dst[rows, :] = nn(s.xt[rows, :], s.dcat[h]).astype(BF16)
                return 0

            lax.fori_loop(0, width // 128, body, 0)
            red["d0" if h == 0 else "d1"].step(0)

        def attend_back(i, _):
            h = lax.div(i, blocks)
            qi = lax.rem(t * (blocks // 2) + lax.rem(i, blocks), blocks)
            rows = blk(qi * qb, qb)
            d_mixed = s.dmix[h, rows, :]
            delta = row_sum((d_mixed.astype(F32) * s.mix[h, rows, :].astype(F32)).T)
            probs = jnp.exp2(block_scores(h, rows) - s.lse[h, :, rows])
            low = probs.astype(BF16)
            s.dvacc[h] += nn(low, d_mixed)
            d_scores = (probs * (nt(s.v[h], d_mixed) - delta)).astype(BF16)
            s.dkacc[h] += nn(d_scores, s.q[h, rows, :])
            dqt = nn(s.kt[h], d_scores) * (HD ** (-0.5))
            s.dcat[h, rows, 0:HD] = dqt.T.astype(BF16)

            @pl.when(i == blocks - 1)
            def _():
                finish_head(0)
                red["a"].step(1)

            @pl.when(i == blocks + 1)
            def _():
                red["b"].step(1)

            @pl.when(i == blocks + 2)
            def _():
                red["a"].step(2)
                red["c"].step(1)

            return 0

        lax.fori_loop(0, n_att, attend_back, 0)
        finish_head(1)
        launch(small_t)
        red["b"].step(2)
        red["d0"].step(1)
        red["c"].step(2)
        red["a"].step(3)
        small_t.wait_recv()
        s.sm0[...] = s.sm[...] + s.smt[...]
        s.sm0[3:4, :] = s.sm[3:4, :] + s.smt[4:5, :]
        s.sm0[8:9, :] = s.sm[8:9, :]
        for c in small_copies(0):
            c.start()

        def project_back(i, _):
            rows = blk(lax.rem(other * (blocks // 2) + i, blocks) * qb, qb)
            wide = jnp.concatenate([s.dcat[h, rows, :] for h in range(heads)], 1)
            wcat = jnp.concatenate(
                [wqkv[c][:, h * HD : (h + 1) * HD] for h in range(heads) for c in range(3)], 1
            )
            return nt(wide, wcat)

        def send_rows(i, _):
            s.dxs[blk(i * qb, qb), :] = project_back(i, 0).astype(BF16)
            return 0

        def keep_rows(i, _):
            s.dpre[blk((i - blocks // 2) * qb, qb), :] += project_back(i, 0)
            return 0

        lax.fori_loop(0, blocks // 2, send_rows, 0)
        launch(dx_out)
        red["b"].step(3)
        red["d0"].step(2)
        red["d1"].step(1)
        red["c"].step(3)
        lax.fori_loop(blocks // 2, blocks, keep_rows, 0)
        red["a"].step(4)
        red["b"].step(4)
        dx_out.wait_recv()
        din_o[...] = (s.dpre[...] + s.dxr[...].astype(F32)).astype(BF16)

        def small_sum(i):
            src, got = small_bufs[i]
            for c in small_copies(i):
                c.wait_recv()
            total = src[...]
            for j in range(axes[i][0] - 1):
                total = total + got[j]
            return total

        red["d1"].step(2)
        s.sm1[...] = small_sum(0)
        for c in small_copies(1):
            c.start()
        red["d0"].step(3)
        red["a"].step(5)
        red["c"].step(4)
        red["b"].step(5)
        red["d1"].step(3)
        s.sm2[...] = small_sum(1)
        for c in small_copies(2):
            c.start()
        red["d0"].step(4)
        red["c"].step(5)
        red["d0"].step(5)
        red["d1"].step(4)
        small_o[...] = small_sum(2)
        red["a"].step(6)
        red["d1"].step(5)
        red["b"].step(6)
        red["c"].step(6)
        red["d0"].step(6)
        red["d1"].step(6)
        for c in all_copies:
            c.wait_send()
        for i in range(3):
            for c in small_copies(i):
                c.wait_send()
        for r in red.values():
            r.drain()

    return kernel, list(scratch.values()), n_sems, grads


def solution(mesh):
    chips = mesh.shape["dp"]
    sizes = torus_sizes(chips)

    def on_device(
        inputs, w_qkv, b_qv, w_out, b_out, norm1_gain, norm1_shift, w_in, b_in, w_down, b_down, norm2_gain, norm2_shift,
        segment_ids, d_out,
    ):
        length, width = inputs.shape
        fh = w_in.shape[1]
        hw = w_out.shape[0]
        kernel, scratch, n_sems, grads = make_kernel(sizes, length, width, 2 * fh)
        row = lambda v: v.reshape(1, -1)
        vmem = pl.BlockSpec(memory_space=pltpu.VMEM)
        half = length // 2
        shapes = [
            jax.ShapeDtypeStruct((half, width), BF16),
            jax.ShapeDtypeStruct((half, width), BF16),
            *[jax.ShapeDtypeStruct((rows, cols), BF16) for _, rows, cols in grads],
            jax.ShapeDtypeStruct((16, width), F32),
        ]
        output, d_inputs, ga, gb, gc, gd0, gd1, small = pl.pallas_call(
            kernel,
            out_shape=shapes,
            in_specs=[vmem] * 15,
            out_specs=[vmem] * len(shapes),
            scratch_shapes=[*scratch, pltpu.SemaphoreType.DMA((n_sems,)), pltpu.SemaphoreType.DMA((n_sems,))],
            compiler_params=pltpu.CompilerParams(
                collective_id=0, has_side_effects=True, vmem_limit_bytes=60 * 1024 * 1024
            ),
        )(
            inputs, w_qkv, b_qv, w_out, row(b_out), row(norm1_gain), row(norm1_shift), w_in, row(b_in), w_down,
            row(b_down), row(norm2_gain), row(norm2_shift), segment_ids, d_out,
        )
        grad_w_qkv = jnp.stack(
            [jnp.concatenate([g[:, c * HD : (c + 1) * HD] for g in (gd0, gd1)], 1) for c in range(3)]
        ).astype(F32)
        return (
            output,
            d_inputs,
            grad_w_qkv,
            small[8].reshape(2, hw),
            gc.astype(F32),
            small[7],
            small[6],
            small[5],
            gb.astype(F32),
            small[3],
            ga.astype(F32),
            small[2],
            small[1],
            small[0],
        )

    placed = (
        P("dp", None),
        P(None, None, "tensor"),
        P(None, "tensor"),
        P("tensor", None),
        P(),
        P(),
        P(),
        P(None, "tensor"),
        P("tensor"),
        P("tensor", None),
        P(),
        P(),
        P(),
        P("dp", None),
        P(("dp", "tensor"), None),
    )
    return jax.shard_map(
        on_device,
        mesh=mesh,
        in_specs=placed,
        out_specs=(
            P(("dp", "tensor"), None),
            P(("dp", "tensor"), None),
            P(None, None, "tensor"),
            P(None, "tensor"),
            P("tensor", None),
            P(),
            P(),
            P(),
            P(None, "tensor"),
            P("tensor"),
            P("tensor", None),
            P(),
            P(),
            P(),
        ),
        check_vma=False,
    )
```

```python
import jax
import jax.numpy as jnp
from jax import lax
from jax.experimental import pallas as pl
from jax.experimental.pallas import tpu as pltpu
from jax.sharding import PartitionSpec as P

HD = 128
NORM_EPSILON = 1e-05
MASKED_SCORE = -1e30
LOG2E = 1.4426950408889634
F32 = jnp.float32
BF16 = jnp.bfloat16
MESH = pl.DeviceIdType.MESH


def nn(a, b):
    return lax.dot_general(a, b, (((1,), (0,)), ((), ())), preferred_element_type=F32)


def nt(a, b):
    return lax.dot_general(a, b, (((1,), (1,)), ((), ())), preferred_element_type=F32)


def tn(a, b):
    return lax.dot_general(a, b, (((0,), (0,)), ((), ())), preferred_element_type=F32)


def torus_sizes(chips):
    side = 1
    for k in range(1, chips + 1):
        if chips % (k * k) == 0 and chips // (k * k) >= k:
            side = k
    return side, side, chips // (side * side)


class Semaphores:
    def __init__(self, send_sem, recv_sem):
        self.count = 0
        self.send, self.recv = send_sem, recv_sem

    def take(self, n=1):
        first = self.count
        self.count += n
        return first


def piece_rows(rows, groups):
    sizes = [rows]
    for n, split in groups:
        sizes.append(sizes[-1] // n if split else sizes[-1])
    return sizes


def reduction_scratch(rows, cols, groups):
    sizes = piece_rows(rows, groups)
    specs = [pltpu.VMEM((n - 1, sizes[i + 1], cols), BF16) for i, (n, _) in enumerate(groups)]
    specs += [pltpu.VMEM((sizes[i + 1], cols), BF16) for i in range(len(groups) - 1)]
    return specs


class Reduction:
    def __init__(self, rows, groups, sems, grad, scratch, out):
        self.groups, self.sems, self.out = groups, sems, out
        count = len(groups)
        self.size = piece_rows(rows, [(n, split) for n, _, _, split in groups])
        self.recv = scratch[:count]
        self.held = [grad, *scratch[count:]]
        self.off = [0]
        for i, (n, place, _, split) in enumerate(groups):
            step = self.size[i + 1]
            self.off.append(pl.multiple_of(self.off[i] + place * step, step) if split else self.off[i])
        self.first = [sems.take(n - 1) for n, _, _, _ in groups]
        self.gathers = [i for i in reversed(range(count)) if groups[i][3]]
        self.gather_first = {i: sems.take(groups[i][0] - 1) for i in self.gathers}
        self.last = count + len(self.gathers)

    def copy(self, i, j, first, src, dst):
        n, place, peer, _ = self.groups[i]
        slot = first + j - 1
        return pltpu.make_async_remote_copy(
            src_ref=src,
            dst_ref=dst,
            send_sem=self.sems.send.at[slot],
            recv_sem=self.sems.recv.at[slot],
            device_id=peer(lax.rem(place + j, n)),
            device_id_type=MESH,
        )

    def scatter(self, i):
        n, place, _, split = self.groups[i]
        size = self.size[i + 1]
        copies = []
        for j in range(1, n):
            src = self.held[i]
            if split:
                src = src.at[pl.ds(pl.multiple_of(lax.rem(place + j, n) * size, size), size)]
            copies.append(self.copy(i, j, self.first[i], src, self.recv[i].at[j - 1]))
        return copies

    def gather(self, i, back):
        n, place, _, _ = self.groups[i]
        size = self.size[i + 1]
        copies = []
        for j in range(1, n):
            owner = lax.rem(place + n - j, n) if back else place
            piece = self.out.at[pl.ds(pl.multiple_of(self.off[i] + owner * size, size), size)]
            copies.append(self.copy(i, j, self.gather_first[i], piece, piece))
        return copies

    def total(self, i):
        n, place, _, split = self.groups[i]
        size = self.size[i + 1]
        for c in self.scatter(i):
            c.wait_recv()
        rows = pl.ds(pl.multiple_of(place * size, size), size) if split else slice(None)
        sum_ = self.held[i][rows, :].astype(F32)
        for j in range(n - 1):
            sum_ = sum_ + self.recv[i][j].astype(F32)
        return sum_.astype(BF16)

    def step(self, number):
        count = len(self.groups)
        if number == 0:
            copies = self.scatter(0)
        elif number < count:
            self.held[number][...] = self.total(number - 1)
            copies = self.scatter(number)
        else:
            done = number - count
            if done == 0:
                self.out[pl.ds(self.off[count], self.size[count]), :] = self.total(count - 1)
            else:
                for c in self.gather(self.gathers[done - 1], True):
                    c.wait_recv()
            copies = self.gather(self.gathers[done], False) if done < len(self.gathers) else []
        for c in copies:
            c.start()

    def drain(self):
        for i in range(len(self.groups)):
            for c in self.scatter(i):
                c.wait_send()
        for i in self.gathers:
            for c in self.gather(i, False):
                c.wait_send()


def blk(start, size, align=None):
    return pl.ds(pl.multiple_of(start, align or size), size)


LOOP = {3: ("d0:0", "a1"), 5: ("b1",), 6: ("a2", "c1")}
TAIL = (
    "head1", "d1:0", "sm0", "b2", "d0:1", "c2", "a3", "sm1", "dx_send", "b3", "d0:2", "d1:1", "c3", "dx_keep", "a4", "b4",
    "dx_end", "d1:2", "sm2", "d0:3", "a5", "c4", "b5", "d1:3", "sm3", "d0:4", "c5", "d0:5", "d1:4", "sm4",
    "a6", "b6", "c6", "d0:6",
)


def make_kernel(sizes, length, width, hidden_units):
    nx, ny, nz = sizes
    half = length // 2
    qb = 256
    fh = hidden_units // 2
    heads = 2
    hw = heads * HD
    kcat = 3 * HD
    blocks = length // qb
    score_c = HD ** (-0.5) * LOG2E

    def split_z(rows):
        return rows % (nx * ny * nz) == 0 and (rows // (nx * ny * nz)) % 16 == 0

    grads = dict(a=(fh, width), b=(width, fh), c=(hw, width), d0=(width, kcat), d1=(width, kcat))
    plane = ("d1",)

    def group_sizes(name):
        z = (nz, split_z(grads[name][0]))
        return [(nx * ny, True), z] if name in plane else [(nx, True), (ny, True), z]

    scratch = dict(
        x=pltpu.VMEM((length, width), BF16),
        wqkv=pltpu.VMEM((3, width, hw), BF16),
        wout=pltpu.VMEM((hw, width), BF16),
        win=pltpu.VMEM((width, fh), BF16),
        wdown=pltpu.VMEM((fh, width), BF16),
        dout=pltpu.VMEM((half, width), BF16),
        output=pltpu.VMEM((half, width), BF16),
        xt=pltpu.VMEM((width, length), BF16),
        q=pltpu.VMEM((heads, length, HD), BF16),
        k=pltpu.VMEM((heads, length, HD), BF16),
        v=pltpu.VMEM((heads, length, HD), BF16),
        kt=pltpu.VMEM((heads, HD, length), BF16),
        vt=pltpu.VMEM((heads, HD, length), BF16),
        segf=pltpu.VMEM((1, length), F32),
        kb=pltpu.VMEM((length, qb), F32),
        weights=pltpu.VMEM((heads, blocks, length, qb), BF16),
        inv=pltpu.VMEM((heads, length, HD), F32),
        mix=pltpu.VMEM((heads, length, HD), BF16),
        mo=pltpu.VMEM((heads, half, HD), BF16),
        wout_o=pltpu.VMEM((hw, width), BF16),
        win_o=pltpu.VMEM((width, fh), BF16),
        wdown_o=pltpu.VMEM((fh, width), BF16),
        bin_o=pltpu.VMEM((1, fh), F32),
        hid=pltpu.VMEM((half, width), BF16),
        act=pltpu.VMEM((2, half, fh), BF16),
        gp=pltpu.VMEM((2, qb, fh), F32),
        ddown=pltpu.VMEM((half, width), BF16),
        dup=pltpu.VMEM((2, half, fh), BF16),
        dattn=pltpu.VMEM((half, width), BF16),
        dpre=pltpu.VMEM((half, width), F32),
        dmix=pltpu.VMEM((heads, length, HD), BF16),
        dmo=pltpu.VMEM((heads, half, HD), BF16),
        dkacc=pltpu.VMEM((heads, length, HD), F32),
        dvacc=pltpu.VMEM((heads, length, HD), F32),
        dcat=pltpu.VMEM((heads, length, kcat), BF16),
        dxs=pltpu.VMEM((half, width), BF16),
        dxr=pltpu.VMEM((half, width), BF16),
        din=pltpu.VMEM((half, width), BF16),
        sm=pltpu.VMEM((16, width), F32),
        smt=pltpu.VMEM((16, width), F32),
        sm0=pltpu.VMEM((16, width), F32),
        sm1=pltpu.VMEM((16, width), F32),
        sm2=pltpu.VMEM((16, width), F32),
        sm3=pltpu.VMEM((16, width), F32),
        smr1=pltpu.VMEM((nx - 1, 16, width), F32),
        smr2=pltpu.VMEM((ny - 1, 16, width), F32),
        smr3=pltpu.VMEM((nz - 1, 16, width), F32),
    )
    n_sems = 4 + 2 * heads + 3 + 1 + 1 + (nx + ny + nz - 3)
    n_local = 2 * blocks + 16
    for name, (rows, cols) in grads.items():
        scratch["g_" + name] = pltpu.VMEM((rows, cols), BF16)
        scratch["o_" + name] = pltpu.VMEM((rows, cols), BF16)
        if name in "abc":
            scratch["gs_" + name] = pltpu.VMEM((rows, cols), BF16)
            scratch["gr_" + name] = pltpu.VMEM((rows, cols), BF16)
        for i, spec in enumerate(reduction_scratch(rows, cols, group_sizes(name))):
            scratch[f"red_{name}_{i}"] = spec
        n_sems += sum((n - 1) * (2 if split else 1) for n, split in group_sizes(name))
    names = list(scratch)

    def kernel(x_h, wqkv_h, bqv, wout_h, bout, n1g, n1s, win_h, bin_, wdown_h, bdown, n2g, n2s, seg, dout_h, *rest):
        out_h, din_h, ga_h, gb_h, gc_h, gd0_h, gd1_h, small_o = rest[:8]
        refs = dict(zip(names, rest[8 : 8 + len(names)]))
        send_sem, recv_sem, local_sem = rest[8 + len(names) :]
        s = type("Scratch", (), refs)
        sems = Semaphores(send_sem, recv_sem)

        dp = lax.axis_index("dp")
        t = lax.axis_index("tensor")
        other = 1 - t
        xi = lax.rem(dp, nx)
        yi = lax.rem(lax.div(dp, nx), ny)
        zi = lax.div(dp, nx * ny)
        qi = lax.rem(dp, nx * ny)
        m1 = xi + t * (yi - xi)
        m2 = yi + t * (xi - yi)
        stride1 = 1 + t * (nx - 1)
        stride2 = nx + t * (1 - nx)
        peer1 = lambda c: (dp + (c - m1) * stride1, t)
        peer2 = lambda c: (dp + (c - m2) * stride2, t)
        peer3 = lambda c: (dp + (c - zi) * (nx * ny), t)
        peer_q = lambda c: (dp + (c - qi), t)

        barrier = pltpu.get_barrier_semaphore()

        def greet(device):
            pl.semaphore_signal(barrier, inc=1, device_id=device, device_id_type=MESH)

        greet((dp, other))
        for n, m, peer in ((nx * ny, qi, peer_q), (nz, zi, peer3)):
            for j in range(1, n):
                greet(peer(lax.rem(m + j, n)))

        local = Semaphores(None, local_sem)

        def load(src, dst):
            c = pltpu.make_async_copy(src, dst, local_sem.at[local.take()])
            c.start()
            return c

        x_in = [None] * blocks
        x_in[0] = load(x_h.at[pl.ds(0, qb)], s.x.at[pl.ds(0, qb)])
        wqkv_in = load(wqkv_h, s.wqkv)
        for i in range(1, blocks):
            x_in[i] = load(x_h.at[pl.ds(i * qb, qb)], s.x.at[pl.ds(i * qb, qb)])
        weights_in = [load(wout_h, s.wout), load(win_h, s.win), load(wdown_h, s.wdown), load(dout_h, s.dout)]
        stores = []

        def store(src, dst):
            stores.append(load(src, dst))

        def across(src, dst, slot=None):
            slot = sems.take() if slot is None else slot
            return pltpu.make_async_remote_copy(
                src_ref=src, dst_ref=dst, send_sem=send_sem.at[slot], recv_sem=recv_sem.at[slot],
                device_id=(dp, other), device_id_type=MESH,
            )

        my0 = pl.multiple_of(t * half, half)
        ot0 = pl.multiple_of(other * half, half)
        all_copies = []

        def launch(*copies):
            for c in copies:
                c.start()
                all_copies.append(c)

        red = {}
        for name, (rows, cols) in grads.items():
            z = (nz, zi, peer3, split_z(rows))
            if name in plane:
                groups = [(nx * ny, qi, peer_q, True), z]
            else:
                groups = [(nx, m1, peer1, True), (ny, m2, peer2, True), z]
            bufs = [refs[f"red_{name}_{i}"] for i in range(2 * len(groups) - 1)]
            red[name] = Reduction(rows, groups, sems, refs["g_" + name], bufs, refs["o_" + name])
        hbm_out = dict(a=ga_h, b=gb_h, c=gc_h, d0=gd0_h, d1=gd1_h)
        at = dict.fromkeys(grads, 0)

        def advance(name, number):
            if number > red[name].last:
                return
            assert at[name] == number
            at[name] += 1
            red[name].step(number)
            if number == red[name].last:
                store(refs["o_" + name], hbm_out[name])

        segf = seg[...].astype(F32)
        s.segf[...] = segf
        for b in range(length // 128):
            rows = jnp.broadcast_to(s.segf[:, b * 128 : (b + 1) * 128], (128, 128)).T
            for c in range(qb // 128):
                s.kb[b * 128 : (b + 1) * 128, c * 128 : (c + 1) * 128] = rows

        def project(rows):
            xb = s.x[rows, :]
            s.xt[:, rows] = xb.T
            qv = nn(xb, s.wqkv[0]) + bqv[0:1, :]
            kv = nn(xb, s.wqkv[1])
            vv = nn(xb, s.wqkv[2]) + bqv[1:2, :]
            ql, kl, vl = qv.astype(BF16), kv.astype(BF16), vv.astype(BF16)
            for h in range(heads):
                cols = slice(h * HD, (h + 1) * HD)
                s.q[h, rows, :] = ql[:, cols]
                s.k[h, rows, :] = kl[:, cols]
                s.v[h, rows, :] = vl[:, cols]
                s.kt[h, :, rows] = kl[:, cols].T
                s.vt[h, :, rows] = vl[:, cols].T

        x_in[0].wait()
        wqkv_in.wait()
        project(pl.ds(0, qb))
        for c in x_in[1:]:
            c.wait()

        def project_rest(i, _):
            project(blk(i * qb, qb))
            return 0

        lax.fori_loop(1, blocks, project_rest, 0)
        pl.semaphore_wait(barrier, 1 + (nx * ny - 1) + (nz - 1))
        weights = [across(wout_h, s.wout_o), across(win_h, s.win_o), across(wdown_h, s.wdown_o), across(bin_, s.bin_o)]
        launch(*weights)

        def attend(i, _):
            h = lax.rem(i, heads)
            qi = lax.rem(other * (blocks // 2) + lax.div(i, heads), blocks)
            rows = blk(qi * qb, qb)
            products = nt(s.k[h], s.q[h, rows, :]) * score_c
            scores = jnp.where(s.kb[...] == s.segf[:, rows], products, MASKED_SCORE)
            top = jnp.max(scores, 0, keepdims=True)
            weights_t = jnp.exp2(scores - top)
            inverse = 1.0 / jnp.sum(weights_t, 0, keepdims=True)
            low = weights_t.astype(BF16)
            s.weights[h, qi] = low
            mixed = nn(s.vt[h], low) * inverse
            s.mix[h, rows, :] = mixed.T.astype(BF16)
            s.inv[h, rows, :] = jnp.broadcast_to(inverse, (HD, qb)).T
            return 0

        n_att = heads * blocks
        lax.fori_loop(0, n_att // 2, attend, 0)
        mix_out = [across(s.mix.at[h, pl.ds(ot0, half)], s.mo.at[h]) for h in range(heads)]
        launch(*mix_out)
        lax.fori_loop(n_att // 2, n_att, attend, 0)
        for c in weights_in:
            c.wait()
        for c in weights + mix_out:
            c.wait_recv()

        s.sm[...] = jnp.zeros_like(s.sm)

        def add_small(row, value):
            s.sm[row : row + 1, :] += value

        def row_sum(value):
            return jnp.sum(value, 0, keepdims=True)

        def norm(v):
            average = jnp.mean(v, -1, keepdims=True)
            centred = v - average
            rs = lax.rsqrt(jnp.mean(centred * centred, -1, keepdims=True) + NORM_EPSILON)
            return centred * rs, rs

        def norm_back(e, n, rs):
            return (e - jnp.mean(e, -1, keepdims=True) - n * jnp.mean(e * n, -1, keepdims=True)) * rs

        halves = ((s.win, bin_, s.wdown, s.wout), (s.win_o, s.bin_o, s.wdown_o, s.wout_o))

        def middle(r, _):
            here = blk(r * qb, qb)
            whole = pl.ds(pl.multiple_of(my0 + r * qb, qb), qb)
            mine = jnp.concatenate([s.mix[h, whole, :] for h in range(heads)], 1)
            theirs = jnp.concatenate([s.mo[h, here, :] for h in range(heads)], 1)
            pre1 = s.x[whole, :].astype(F32) + (nn(mine, s.wout[...]) + nn(theirs, s.wout_o[...]) + bout[...])
            n1, rs1 = norm(pre1)
            hidden = n1 * n1g[...] + n1s[...]
            low = hidden.astype(BF16)
            s.hid[here, :] = low
            for f, (w_in, b_in, _, _) in enumerate(halves):
                up = nn(low, w_in[...]) + b_in[...]
                cdf = 0.5 * (1.0 + lax.erf(up * (0.5**0.5)))
                s.act[f, here, :] = (up * cdf).astype(BF16)
                s.gp[f] = cdf + up * (jnp.exp2(up * up * (-0.5 * LOG2E)) * 0.3989422804014327)
            down = nn(s.act[0, here, :], s.wdown[...]) + nn(s.act[1, here, :], s.wdown_o[...]) + bdown[...]
            n2, rs2 = norm(hidden + down)
            row_mask = (s.kb[whole, 0:1] != 0.0).astype(F32)
            s.output[here, :] = ((n2 * n2g[...] + n2s[...]) * row_mask).astype(BF16)
            cot = s.dout[here, :].astype(F32) * row_mask
            add_small(0, row_sum(cot))
            add_small(1, row_sum(cot * n2))
            d_resid = norm_back(cot * n2g[...], n2, rs2)
            d_down = d_resid.astype(BF16)
            s.ddown[here, :] = d_down
            add_small(2, row_sum(d_down.astype(F32)))
            d_hidden = d_resid
            for f, (w_in, _, w_down, _) in enumerate(halves):
                d_up = (nt(d_down, w_down[...]) * s.gp[f]).astype(BF16)
                s.dup[f, here, :] = d_up
                add_small(3 + f, row_sum(d_up.astype(F32)))
                d_hidden = d_hidden + nt(d_up, w_in[...])
            add_small(5, row_sum(d_hidden))
            add_small(6, row_sum(d_hidden * n1))
            d_pre = norm_back(d_hidden * n1g[...], n1, rs1)
            s.dpre[here, :] = d_pre
            d_attn = d_pre.astype(BF16)
            s.dattn[here, :] = d_attn
            add_small(7, row_sum(d_attn.astype(F32)))
            dm = nt(d_attn, s.wout[...]).astype(BF16)
            do = nt(d_attn, s.wout_o[...]).astype(BF16)
            for h in range(heads):
                s.dmix[h, whole, :] = dm[:, h * HD : (h + 1) * HD]
                s.dmo[h, here, :] = do[:, h * HD : (h + 1) * HD]
            return 0

        lax.fori_loop(0, half // qb, middle, 0)
        dmix_slots = [sems.take() for _ in range(heads)]
        launch(*[across(s.dmo.at[h], s.dmix.at[h, pl.ds(my0, half)], dmix_slots[h]) for h in range(heads)])
        store(s.output, out_h)

        def grad_block(dst, lhs, rhs):
            def body(i, _):
                cols = blk(i * qb, qb)
                dst[cols, :] = tn(lhs[:, cols], rhs[...]).astype(BF16)
                return 0

            lax.fori_loop(0, lhs.shape[1] // qb, body, 0)

        part = {name: across(refs["gs_" + name], refs["gr_" + name]) for name in "abc"}

        def join(name):
            part[name].wait_recv()
            mine, theirs = refs["g_" + name], refs["gr_" + name]
            mine[...] = (mine[...].astype(F32) + theirs[...].astype(F32)).astype(BF16)
            advance(name, 0)

        grad_block(s.gs_a, s.act.at[1], s.ddown)
        launch(part["a"])
        grad_block(s.g_a, s.act.at[0], s.ddown)
        grad_block(s.gs_b, s.hid, s.dup.at[1])
        launch(part["b"])
        join("a")
        grad_block(s.g_b, s.hid, s.dup.at[0])
        theirs = jnp.concatenate([s.mo[h] for h in range(heads)], 1)
        s.gs_c[...] = tn(theirs, s.dattn[...]).astype(BF16)
        launch(part["c"])
        join("b")
        mine = jnp.concatenate([s.mix[h, pl.ds(my0, half), :] for h in range(heads)], 1)
        s.g_c[...] = tn(mine, s.dattn[...]).astype(BF16)
        join("c")

        s.dkacc[...] = jnp.zeros_like(s.dkacc)
        s.dvacc[...] = jnp.zeros_like(s.dvacc)
        for h in range(heads):
            across(s.dmo.at[h], s.dmix.at[h, pl.ds(ot0, half)], dmix_slots[h]).wait_recv()

        def finish_head(h):
            dk = (s.dkacc[h] * (HD ** (-0.5))).astype(BF16)
            dv = s.dvacc[h].astype(BF16)
            s.dcat[h, :, HD : 2 * HD] = dk
            s.dcat[h, :, 2 * HD :] = dv
            s.sm[8:9, h * HD : (h + 1) * HD] = row_sum(s.dcat[h, :, 0:HD].astype(F32))
            s.sm[8:9, hw + h * HD : hw + (h + 1) * HD] = row_sum(dv.astype(F32))
            dst = s.g_d0 if h == 0 else s.g_d1

            def body(i, _):
                rows = blk(i * 128, 128)
                dst[rows, :] = nn(s.xt[rows, :], s.dcat[h]).astype(BF16)
                return 0

            lax.fori_loop(0, width // 128, body, 0)

        def advance_all(tokens):
            for token in tokens:
                name, number = token.split(":") if ":" in token else (token[0], token[1:])
                advance(name, int(number))

        def attend_back(i, _):
            h = lax.div(i, blocks)
            qi = lax.rem(t * (blocks // 2) + lax.rem(i, blocks), blocks)
            rows = blk(qi * qb, qb)
            d_mixed = s.dmix[h, rows, :].astype(F32) * s.inv[h, rows, :]
            delta = row_sum((d_mixed * s.mix[h, rows, :].astype(F32)).T)
            d_low = d_mixed.astype(BF16)
            weights_t = s.weights[h, qi]
            s.dvacc[h] += nn(weights_t, d_low)
            d_scores = (weights_t.astype(F32) * (nt(s.v[h], d_low) - delta)).astype(BF16)
            s.dkacc[h] += nn(d_scores, s.q[h, rows, :])
            dqt = nn(s.kt[h], d_scores) * (HD ** (-0.5))
            s.dcat[h, rows, 0:HD] = dqt.T.astype(BF16)
            for number, tokens in LOOP.items():

                @pl.when(i == number)
                def _():
                    if number == blocks - 1:
                        finish_head(0)
                    advance_all(tokens)

            return 0

        lax.fori_loop(0, n_att, attend_back, 0)

        def project_back(i):
            rows = blk(lax.rem(other * (blocks // 2) + i, blocks) * qb, qb)
            wide = jnp.concatenate([s.dcat[h, rows, :] for h in range(heads)], 1)
            wcat = jnp.concatenate(
                [s.wqkv[c][:, h * HD : (h + 1) * HD] for h in range(heads) for c in range(3)], 1
            )
            return nt(wide, wcat)

        def send_rows(i, _):
            s.dxs[blk(i * qb, qb), :] = project_back(i).astype(BF16)
            return 0

        def keep_rows(i, _):
            s.dpre[blk((i - blocks // 2) * qb, qb), :] += project_back(i)
            return 0

        dx_out = across(s.dxs, s.dxr)
        small_t = across(s.sm, s.smt)
        small_groups = ((nx, m1, peer1), (ny, m2, peer2), (nz, zi, peer3))
        small_bufs = ((s.sm0, s.smr1, s.sm1), (s.sm1, s.smr2, s.sm2), (s.sm2, s.smr3, s.sm3))
        small_first = [sems.take(n - 1) for n, _, _ in small_groups]
        assert sems.count == n_sems

        def small_copies(i):
            n, m, peer = small_groups[i]
            src, dst, _ = small_bufs[i]
            return [
                pltpu.make_async_remote_copy(
                    src_ref=src, dst_ref=dst.at[j - 1], send_sem=send_sem.at[small_first[i] + j - 1],
                    recv_sem=recv_sem.at[small_first[i] + j - 1], device_id=peer(lax.rem(m + j, n)), device_id_type=MESH,
                )
                for j in range(1, n)
            ]

        def small_step(number):
            if number == 0:
                launch(small_t)
                return
            if number == 1:
                small_t.wait_recv()
                s.sm0[...] = s.sm[...] + s.smt[...]
                s.sm0[3:4, :] = s.sm[3:4, :] + s.smt[4:5, :]
                s.sm0[8:9, :] = s.sm[8:9, :]
            else:
                src, got, dst = small_bufs[number - 2]
                for c in small_copies(number - 2):
                    c.wait_recv()
                total = src[...]
                for j in range(small_groups[number - 2][0] - 1):
                    total = total + got[j]
                dst[...] = total
            if number <= 3:
                for c in small_copies(number - 1):
                    c.start()
            else:
                small_o[...] = s.sm3[...]

        for token in TAIL:
            if token == "head1":
                finish_head(1)
            elif token == "dx_send":
                lax.fori_loop(0, blocks // 2, send_rows, 0)
                launch(dx_out)
            elif token == "dx_keep":
                lax.fori_loop(blocks // 2, blocks, keep_rows, 0)
            elif token == "dx_end":
                dx_out.wait_recv()
                s.din[...] = (s.dpre[...] + s.dxr[...].astype(F32)).astype(BF16)
                store(s.din, din_h)
            elif token.startswith("sm"):
                small_step(int(token[2:]))
            else:
                advance_all([token])
        for name in grads:
            while at[name] <= red[name].last:
                advance(name, at[name])
        for c in all_copies:
            c.wait_send()
        for i in range(3):
            for c in small_copies(i):
                c.wait_send()
        for r in red.values():
            r.drain()
        for c in stores:
            c.wait()

    return kernel, list(scratch.values()), n_sems, n_local, grads


def finish_kernel(grads, half, width, hw):
    def kernel(out_i, din_i, ga, gb, gc, gd0, gd1, small, out_o, din_o, gqkv_o, gout_o, gin_o, gdown_o, bqv_o, *rest):
        rows_o, (v_out, v_din, va, vb, vc, vd0, vd1, fa, fb, fc, fqkv, sems) = rest[:7], rest[7:]
        loads = [
            pltpu.make_async_copy(src, dst, sems.at[i])
            for i, (src, dst) in enumerate(
                ((ga, va), (gb, vb), (gd0, vd0), (gd1, vd1), (gc, vc), (out_i, v_out), (din_i, v_din))
            )
        ]
        stores = [
            pltpu.make_async_copy(src, dst, sems.at[8 + i])
            for i, (src, dst) in enumerate(
                ((fa, gdown_o), (fb, gin_o), (fqkv, gqkv_o), (fc, gout_o), (v_out, out_o), (v_din, din_o))
            )
        ]
        for c in loads:
            c.start()
        for row, ref in zip((7, 6, 5, 3, 2, 1, 0), rows_o):
            ref[...] = small[row : row + 1, :]
        for i in range(2):
            bqv_o[i : i + 1, :] = small[8:9, i * hw : (i + 1) * hw]
        loads[0].wait()
        fa[...] = va[...].astype(F32)
        stores[0].start()
        loads[1].wait()
        fb[...] = vb[...].astype(F32)
        stores[1].start()
        for h, (load, src) in enumerate(((loads[2], vd0), (loads[3], vd1))):
            load.wait()
            for c in range(3):
                fqkv[c, :, h * HD : (h + 1) * HD] = src[:, c * HD : (c + 1) * HD].astype(F32)
        stores[2].start()
        loads[4].wait()
        fc[...] = vc[...].astype(F32)
        stores[3].start()
        loads[5].wait()
        stores[4].start()
        loads[6].wait()
        stores[5].start()
        for c in stores:
            c.wait()

    fh = grads["a"][0]
    shapes = [
        jax.ShapeDtypeStruct((half, width), BF16),
        jax.ShapeDtypeStruct((half, width), BF16),
        jax.ShapeDtypeStruct((3, width, hw), F32),
        jax.ShapeDtypeStruct((hw, width), F32),
        jax.ShapeDtypeStruct((width, fh), F32),
        jax.ShapeDtypeStruct((fh, width), F32),
        jax.ShapeDtypeStruct((2, hw), F32),
        *[jax.ShapeDtypeStruct((1, width), F32)] * 7,
    ]
    any_ = pl.BlockSpec(memory_space=pl.ANY)
    vmem = pl.BlockSpec(memory_space=pltpu.VMEM)
    vm = pltpu.VMEM
    return pl.pallas_call(
        kernel,
        out_shape=shapes,
        in_specs=[any_] * 7 + [vmem],
        out_specs=[any_] * 6 + [vmem] * 8,
        scratch_shapes=[
            vm((half, width), BF16),
            vm((half, width), BF16),
            *[vm(grads[n], BF16) for n in grads],
            *[vm(grads[n], F32) for n in "abc"],
            vm((3, width, hw), F32),
            pltpu.SemaphoreType.DMA((16,)),
        ],
        compiler_params=pltpu.CompilerParams(vmem_limit_bytes=63 * 1024 * 1024),
    )


def solution(mesh):
    chips = mesh.shape["dp"]
    sizes = torus_sizes(chips)

    def on_device(
        inputs, w_qkv, b_qv, w_out, b_out, norm1_gain, norm1_shift, w_in, b_in, w_down, b_down, norm2_gain, norm2_shift,
        segment_ids, d_out,
    ):
        length, width = inputs.shape
        fh = w_in.shape[1]
        hw = w_out.shape[0]
        half = length // 2
        kernel, scratch, n_sems, n_local, grads = make_kernel(sizes, length, width, 2 * fh)
        row = lambda v: v.reshape(1, -1)
        vmem = pl.BlockSpec(memory_space=pltpu.VMEM)
        any_ = pl.BlockSpec(memory_space=pl.ANY)
        shapes = [
            jax.ShapeDtypeStruct((half, width), BF16),
            jax.ShapeDtypeStruct((half, width), BF16),
            *[jax.ShapeDtypeStruct(shape, BF16) for shape in grads.values()],
            jax.ShapeDtypeStruct((16, width), F32),
        ]
        dma = pltpu.SemaphoreType.DMA
        partial_results = pl.pallas_call(
            kernel,
            out_shape=shapes,
            in_specs=[any_, any_, vmem, any_, vmem, vmem, vmem, any_, vmem, any_, vmem, vmem, vmem, vmem, any_],
            out_specs=[any_] * 7 + [vmem],
            scratch_shapes=[*scratch, dma((n_sems,)), dma((n_sems,)), dma((n_local,))],
            compiler_params=pltpu.CompilerParams(
                collective_id=0, has_side_effects=True, vmem_limit_bytes=60 * 1024 * 1024
            ),
        )(
            inputs, w_qkv, b_qv, w_out, row(b_out), row(norm1_gain), row(norm1_shift), w_in, row(b_in), w_down,
            row(b_down), row(norm2_gain), row(norm2_shift), segment_ids, d_out,
        )
        output, d_inputs, g_qkv, g_out, g_in, g_down, g_bqv, *rows = finish_kernel(grads, half, width, hw)(*partial_results)
        g_bout, g_n1g, g_n1s, g_bin, g_bdown, g_n2g, g_n2s = [v.reshape(-1) for v in rows]
        return (
            output, d_inputs, g_qkv, g_bqv, g_out, g_bout, g_n1g, g_n1s, g_in, g_bin, g_down, g_bdown, g_n2g, g_n2s,
        )

    placed = (
        P("dp", None),
        P(None, None, "tensor"),
        P(None, "tensor"),
        P("tensor", None),
        P(),
        P(),
        P(),
        P(None, "tensor"),
        P("tensor"),
        P("tensor", None),
        P(),
        P(),
        P(),
        P("dp", None),
        P(("dp", "tensor"), None),
    )
    return jax.shard_map(
        on_device,
        mesh=mesh,
        in_specs=placed,
        out_specs=(
            P(("dp", "tensor"), None),
            P(("dp", "tensor"), None),
            P(None, None, "tensor"),
            P(None, "tensor"),
            P("tensor", None),
            P(),
            P(),
            P(),
            P(None, "tensor"),
            P("tensor"),
            P("tensor", None),
            P(),
            P(),
            P(),
        ),
        check_vma=False,
    )
```

```python
import jax
import jax.numpy as jnp
from jax import lax
from jax.experimental import pallas as pl
from jax.experimental.pallas import tpu as pltpu
from jax.sharding import PartitionSpec as P

HD = 128
NORM_EPSILON = 1e-05
MASKED_SCORE = -1e30
LOG2E = 1.4426950408889634
F32 = jnp.float32
BF16 = jnp.bfloat16
MESH = pl.DeviceIdType.MESH


def nn(a, b):
    return lax.dot_general(a, b, (((1,), (0,)), ((), ())), preferred_element_type=F32)


def nt(a, b):
    return lax.dot_general(a, b, (((1,), (1,)), ((), ())), preferred_element_type=F32)


def tn(a, b):
    return lax.dot_general(a, b, (((0,), (0,)), ((), ())), preferred_element_type=F32)


def torus_sizes(chips):
    side = 1
    for k in range(1, chips + 1):
        if chips % (k * k) == 0 and chips // (k * k) >= k:
            side = k
    return side, side, chips // (side * side)


class Semaphores:
    def __init__(self, send_sem, recv_sem):
        self.count = 0
        self.send, self.recv = send_sem, recv_sem

    def take(self, n=1):
        first = self.count
        self.count += n
        return first


def piece_rows(rows, groups):
    sizes = [rows]
    for n, split in groups:
        sizes.append(sizes[-1] // n if split else sizes[-1])
    return sizes


def reduction_scratch(rows, cols, groups):
    sizes = piece_rows(rows, groups)
    specs = [pltpu.VMEM((n - 1, sizes[i + 1], cols), BF16) for i, (n, _) in enumerate(groups)]
    specs += [pltpu.VMEM((sizes[i + 1], cols), BF16) for i in range(len(groups) - 1)]
    return specs


class Reduction:
    def __init__(self, rows, groups, sems, grad, scratch, out):
        self.groups, self.sems, self.out = groups, sems, out
        count = len(groups)
        self.size = piece_rows(rows, [(n, split) for n, _, _, split in groups])
        self.recv = scratch[:count]
        self.held = [grad, *scratch[count:]]
        self.off = [0]
        for i, (n, place, _, split) in enumerate(groups):
            step = self.size[i + 1]
            self.off.append(pl.multiple_of(self.off[i] + place * step, step) if split else self.off[i])
        self.slot = [sems.take() for _ in groups]
        self.gathers = [i for i in reversed(range(count)) if groups[i][3]]
        self.gather_slot = {i: sems.take() for i in self.gathers}
        self.last = count + len(self.gathers)

    def copy(self, i, j, slot, src, dst):
        n, place, peer, _ = self.groups[i]
        return pltpu.make_async_remote_copy(
            src_ref=src,
            dst_ref=dst,
            send_sem=self.sems.send.at[slot],
            recv_sem=self.sems.recv.at[slot],
            device_id=peer(lax.rem(place + j, n)),
            device_id_type=MESH,
        )

    def scatter(self, i):
        n, place, _, split = self.groups[i]
        size = self.size[i + 1]
        copies = []
        for j in range(1, n):
            src = self.held[i]
            if split:
                src = src.at[pl.ds(pl.multiple_of(lax.rem(place + j, n) * size, size), size)]
            copies.append(self.copy(i, j, self.slot[i], src, self.recv[i].at[j - 1]))
        return copies

    def gather(self, i):
        n, place, _, _ = self.groups[i]
        size = self.size[i + 1]
        piece = self.out.at[pl.ds(pl.multiple_of(self.off[i] + place * size, size), size)]
        return [self.copy(i, j, self.gather_slot[i], piece, piece) for j in range(1, n)]

    def all_of(self, i, slot):
        return self.copy(i, 1, slot, self.recv[i], self.recv[i])

    def total(self, i):
        n, place, _, split = self.groups[i]
        size = self.size[i + 1]
        self.all_of(i, self.slot[i]).wait_recv()
        rows = pl.ds(pl.multiple_of(place * size, size), size) if split else slice(None)
        sum_ = self.held[i][rows, :].astype(F32)
        for j in range(n - 1):
            sum_ = sum_ + self.recv[i][j].astype(F32)
        return sum_.astype(BF16)

    def step(self, number):
        count = len(self.groups)
        if number == 0:
            copies = self.scatter(0)
        elif number < count:
            self.held[number][...] = self.total(number - 1)
            copies = self.scatter(number)
        else:
            done = number - count
            if done == 0:
                self.out[pl.ds(self.off[count], self.size[count]), :] = self.total(count - 1)
            else:
                last = self.gathers[done - 1]
                self.all_of(last, self.gather_slot[last]).wait_recv()
            copies = self.gather(self.gathers[done]) if done < len(self.gathers) else []
        for c in copies:
            c.start()

    def drain(self):
        for i in range(len(self.groups)):
            self.all_of(i, self.slot[i]).wait_send()
        for i in self.gathers:
            self.all_of(i, self.gather_slot[i]).wait_send()


def blk(start, size, align=None):
    return pl.ds(pl.multiple_of(start, align or size), size)


LOOP = {
    1: ("a.0:1",),
    2: ("a.1:1",),
    3: ("head0", "b.0:1", "a.0:2"),
    4: ("a.1:2", "b.1:1"),
    6: ("c.0:1", "c.1:1", "d0.0:1", "b.0:2"),
    7: ("d0.1:1", "b.1:2"),
}
TAIL = (
    "head1", "d0.2:1", "a.0:3", "d0.0:2", "a.1:3", "sm0", "dx_send", "d0.1:2", "c.0:2", "sm1", "dx_keep", "dx_end",
    "sm2", "c.1:2", "b.0:3", "d1.0:1", "b.1:3", "d1.1:1", "d0.2:2", "a.0:4", "d1.2:1", "sm3", "d0.0:3", "a.1:4",
    "d0.1:3", "c.0:3", "a.0:5", "c.1:3", "b.0:4", "a.1:5", "d1.0:2", "b.1:4", "c.0:4", "d1.1:2", "sm4", "d0.2:3",
    "d1.2:2", "a.0:6", "b.0:5", "d0.0:4", "d0.1:4", "c.1:4", "b.1:5", "d1.0:3", "a.1:6", "d1.1:3", "d0.0:5", "d0.2:4",
    "d0.1:5", "b.0:6", "d1.2:3", "b.1:6", "d0.2:5", "d1.0:4", "d1.1:4", "d0.0:6", "d0.1:6", "d0.2:6", "d1.2:4",
)
PARTS = dict(a=2, b=2, c=2, d0=3, d1=3)


def make_kernel(sizes, length, width, hidden_units):
    nx, ny, nz = sizes
    half = length // 2
    qb = 256
    fh = hidden_units // 2
    heads = 2
    hw = heads * HD
    kcat = 3 * HD
    blocks = length // qb
    score_c = HD ** (-0.5) * LOG2E

    def split_z(rows):
        return rows % (nx * ny * nz) == 0 and (rows // (nx * ny * nz)) % 16 == 0

    grads = dict(a=(fh, width), b=(width, fh), c=(hw, width), d0=(width, kcat), d1=(width, kcat))
    plane = ("c", "d1")

    def group_sizes(name):
        z = (nz, split_z(grads[name][0]))
        return [(nx * ny, True), z] if name in plane else [(nx, True), (ny, True), z]

    scratch = dict(
        x=pltpu.VMEM((length, width), BF16),
        wqkv=pltpu.VMEM((3, width, hw), BF16),
        wout=pltpu.VMEM((hw, width), BF16),
        win=pltpu.VMEM((width, fh), BF16),
        wdown=pltpu.VMEM((fh, width), BF16),
        dout=pltpu.VMEM((half, width), BF16),
        output=pltpu.VMEM((half, width), BF16),
        xt=pltpu.VMEM((width, length), BF16),
        q=pltpu.VMEM((heads, length, HD), BF16),
        k=pltpu.VMEM((heads, length, HD), BF16),
        v=pltpu.VMEM((heads, length, HD), BF16),
        kt=pltpu.VMEM((heads, HD, length), BF16),
        vt=pltpu.VMEM((heads, HD, length), BF16),
        segf=pltpu.VMEM((1, length), F32),
        kb=pltpu.VMEM((length, qb), F32),
        weights=pltpu.VMEM((heads, blocks, length, qb), BF16),
        inv=pltpu.VMEM((heads, length, HD), F32),
        mix=pltpu.VMEM((heads, length, HD), BF16),
        mo=pltpu.VMEM((heads, half, HD), BF16),
        wout_o=pltpu.VMEM((hw, width), BF16),
        win_o=pltpu.VMEM((width, fh), BF16),
        wdown_o=pltpu.VMEM((fh, width), BF16),
        bin_o=pltpu.VMEM((1, fh), F32),
        hid=pltpu.VMEM((half, width), BF16),
        act=pltpu.VMEM((2, half, fh), BF16),
        gp=pltpu.VMEM((2, qb, fh), F32),
        ddown=pltpu.VMEM((half, width), BF16),
        dup=pltpu.VMEM((2, half, fh), BF16),
        dattn=pltpu.VMEM((half, width), BF16),
        dpre=pltpu.VMEM((half, width), F32),
        dmix=pltpu.VMEM((heads, length, HD), BF16),
        dmo=pltpu.VMEM((heads, half, HD), BF16),
        dkacc=pltpu.VMEM((heads, length, HD), F32),
        dvacc=pltpu.VMEM((heads, length, HD), F32),
        dcat=pltpu.VMEM((heads, length, kcat), BF16),
        dxs=pltpu.VMEM((half, width), BF16),
        dxr=pltpu.VMEM((half, width), BF16),
        din=pltpu.VMEM((half, width), BF16),
        sm=pltpu.VMEM((16, width), F32),
        smt=pltpu.VMEM((16, width), F32),
        sm0=pltpu.VMEM((16, width), F32),
        sm1=pltpu.VMEM((16, width), F32),
        sm2=pltpu.VMEM((16, width), F32),
        sm3=pltpu.VMEM((16, width), F32),
        smr1=pltpu.VMEM((nx - 1, 16, width), F32),
        smr2=pltpu.VMEM((ny - 1, 16, width), F32),
        smr3=pltpu.VMEM((nz - 1, 16, width), F32),
    )
    n_sems = 4 + 2 * heads + 3 + 1 + 1 + (nx + ny + nz - 3)
    n_local = 2 * blocks + 16
    for name, (rows, cols) in grads.items():
        scratch["g_" + name] = pltpu.VMEM((rows, cols), BF16)
        scratch["o_" + name] = pltpu.VMEM((rows, cols), BF16)
        if name in "abc":
            scratch["gs_" + name] = pltpu.VMEM((rows, cols), BF16)
            scratch["gr_" + name] = pltpu.VMEM((rows, cols), BF16)
        for p in range(PARTS[name]):
            for i, spec in enumerate(reduction_scratch(rows, cols // PARTS[name], group_sizes(name))):
                scratch[f"red_{name}.{p}_{i}"] = spec
            n_sems += sum(2 if split else 1 for _, split in group_sizes(name))
    names = list(scratch)

    def kernel(x_h, wqkv_h, bqv, wout_h, bout, n1g, n1s, win_h, bin_, wdown_h, bdown, n2g, n2s, seg, dout_h, *rest):
        out_h, din_h, ga_h, gb_h, gc_h, gd0_h, gd1_h, small_o = rest[:8]
        refs = dict(zip(names, rest[8 : 8 + len(names)]))
        send_sem, recv_sem, local_sem = rest[8 + len(names) :]
        s = type("Scratch", (), refs)
        sems = Semaphores(send_sem, recv_sem)

        dp = lax.axis_index("dp")
        t = lax.axis_index("tensor")
        other = 1 - t
        xi = lax.rem(dp, nx)
        yi = lax.rem(lax.div(dp, nx), ny)
        zi = lax.div(dp, nx * ny)
        qi = lax.rem(dp, nx * ny)
        m1 = xi + t * (yi - xi)
        m2 = yi + t * (xi - yi)
        stride1 = 1 + t * (nx - 1)
        stride2 = nx + t * (1 - nx)
        peer1 = lambda c: (dp + (c - m1) * stride1, t)
        peer2 = lambda c: (dp + (c - m2) * stride2, t)
        peer3 = lambda c: (dp + (c - zi) * (nx * ny), t)
        peer_q = lambda c: (dp + (c - qi), t)

        barrier = pltpu.get_barrier_semaphore()

        def greet(device):
            pl.semaphore_signal(barrier, inc=1, device_id=device, device_id_type=MESH)

        greet((dp, other))
        for n, m, peer in ((nx * ny, qi, peer_q), (nz, zi, peer3)):
            for j in range(1, n):
                greet(peer(lax.rem(m + j, n)))

        local = Semaphores(None, local_sem)

        def load(src, dst):
            c = pltpu.make_async_copy(src, dst, local_sem.at[local.take()])
            c.start()
            return c

        x_in = [None] * blocks
        x_in[0] = load(x_h.at[pl.ds(0, qb)], s.x.at[pl.ds(0, qb)])
        wqkv_in = load(wqkv_h, s.wqkv)
        for i in range(1, blocks):
            x_in[i] = load(x_h.at[pl.ds(i * qb, qb)], s.x.at[pl.ds(i * qb, qb)])
        weights_in = [load(wout_h, s.wout), load(win_h, s.win), load(wdown_h, s.wdown), load(dout_h, s.dout)]
        stores = []

        def store(src, dst):
            stores.append(load(src, dst))

        def across(src, dst, slot=None):
            slot = sems.take() if slot is None else slot
            return pltpu.make_async_remote_copy(
                src_ref=src, dst_ref=dst, send_sem=send_sem.at[slot], recv_sem=recv_sem.at[slot],
                device_id=(dp, other), device_id_type=MESH,
            )

        my0 = pl.multiple_of(t * half, half)
        ot0 = pl.multiple_of(other * half, half)
        all_copies = []

        def launch(*copies):
            for c in copies:
                c.start()
                all_copies.append(c)

        red = {}
        for name, (rows, cols) in grads.items():
            z = (nz, zi, peer3, split_z(rows))
            if name in plane:
                groups = [(nx * ny, qi, peer_q, True), z]
            else:
                groups = [(nx, m1, peer1, True), (ny, m2, peer2, True), z]
            for p in range(PARTS[name]):
                bufs = [refs[f"red_{name}.{p}_{i}"] for i in range(2 * len(groups) - 1)]
                here = pl.ds(p * (cols // PARTS[name]), cols // PARTS[name])
                grad, out = refs["g_" + name].at[:, here], refs["o_" + name].at[:, here]
                red[f"{name}.{p}"] = Reduction(rows, groups, sems, grad, bufs, out)
        hbm_out = dict(a=ga_h, b=gb_h, c=gc_h, d0=gd0_h, d1=gd1_h)
        at = dict.fromkeys(red, 0)

        def advance(name, number):
            if number > red[name].last:
                return
            assert at[name] == number
            at[name] += 1
            red[name].step(number)
            if number == red[name].last:
                parent, p = name.split(".")
                cols = grads[parent][1] // PARTS[parent]
                store(red[name].out, hbm_out[parent].at[:, pl.ds(int(p) * cols, cols)])

        def begin(parent):
            for p in range(PARTS[parent]):
                advance(f"{parent}.{p}", 0)

        segf = seg[...].astype(F32)
        s.segf[...] = segf
        for b in range(length // 128):
            rows = jnp.broadcast_to(s.segf[:, b * 128 : (b + 1) * 128], (128, 128)).T
            for c in range(qb // 128):
                s.kb[b * 128 : (b + 1) * 128, c * 128 : (c + 1) * 128] = rows

        def project(rows):
            xb = s.x[rows, :]
            qv = (nn(xb, s.wqkv[0]) + bqv[0:1, :]) * score_c
            kv = nn(xb, s.wqkv[1])
            vv = nn(xb, s.wqkv[2]) + bqv[1:2, :]
            ql, kl, vl = qv.astype(BF16), kv.astype(BF16), vv.astype(BF16)
            for h in range(heads):
                cols = slice(h * HD, (h + 1) * HD)
                s.q[h, rows, :] = ql[:, cols]
                s.k[h, rows, :] = kl[:, cols]
                s.v[h, rows, :] = vl[:, cols]
                s.vt[h, :, rows] = vl[:, cols].T

        x_in[0].wait()
        wqkv_in.wait()
        project(pl.ds(0, qb))
        for c in x_in[1:]:
            c.wait()

        def project_rest(i, _):
            project(blk(i * qb, qb))
            return 0

        lax.fori_loop(1, blocks, project_rest, 0)
        pl.semaphore_wait(barrier, 1 + (nx * ny - 1) + (nz - 1))
        weights = [across(wout_h, s.wout_o), across(win_h, s.win_o), across(wdown_h, s.wdown_o), across(bin_, s.bin_o)]
        launch(*weights)

        def attend_head(h, qi):
            rows = blk(qi * qb, qb)
            scores = jnp.where(s.kb[...] == s.segf[:, rows], nt(s.k[h], s.q[h, rows, :]), MASKED_SCORE)
            top = jnp.max(scores, 0, keepdims=True)
            weights_t = jnp.exp2(scores - top)
            inverse = 1.0 / jnp.sum(weights_t, 0, keepdims=True)
            low = weights_t.astype(BF16)
            s.weights[h, qi] = low
            mixed = nn(s.vt[h], low) * inverse
            s.mix[h, rows, :] = mixed.T.astype(BF16)
            s.inv[h, rows, :] = jnp.broadcast_to(inverse, (HD, qb)).T

        def attend(i, _):
            for h in range(heads):
                attend_head(h, lax.rem(other * (blocks // 2) + i, blocks))
            return 0

        n_att = heads * blocks
        lax.fori_loop(0, blocks // 2, attend, 0)
        mix_out = [across(s.mix.at[h, pl.ds(ot0, half)], s.mo.at[h]) for h in range(heads)]
        launch(*mix_out)
        lax.fori_loop(blocks // 2, blocks, attend, 0)
        for c in weights_in:
            c.wait()
        for c in weights + mix_out:
            c.wait_recv()

        s.sm[...] = jnp.zeros_like(s.sm)

        def add_small(row, value):
            s.sm[row : row + 1, :] += value

        def row_sum(value):
            return jnp.sum(value, 0, keepdims=True)

        def norm(v):
            average = jnp.mean(v, -1, keepdims=True)
            centred = v - average
            rs = lax.rsqrt(jnp.mean(centred * centred, -1, keepdims=True) + NORM_EPSILON)
            return centred * rs, rs

        def norm_back(e, n, rs):
            return (e - jnp.mean(e, -1, keepdims=True) - n * jnp.mean(e * n, -1, keepdims=True)) * rs

        halves = ((s.win, bin_, s.wdown, s.wout), (s.win_o, s.bin_o, s.wdown_o, s.wout_o))

        def middle(r, _):
            here = blk(r * qb, qb)
            whole = pl.ds(pl.multiple_of(my0 + r * qb, qb), qb)
            mine = jnp.concatenate([s.mix[h, whole, :] for h in range(heads)], 1)
            theirs = jnp.concatenate([s.mo[h, here, :] for h in range(heads)], 1)
            pre1 = s.x[whole, :].astype(F32) + (nn(mine, s.wout[...]) + nn(theirs, s.wout_o[...]) + bout[...])
            n1, rs1 = norm(pre1)
            hidden = n1 * n1g[...] + n1s[...]
            low = hidden.astype(BF16)
            s.hid[here, :] = low
            for f, (w_in, b_in, _, _) in enumerate(halves):
                up = nn(low, w_in[...]) + b_in[...]
                cdf = 0.5 * (1.0 + lax.erf(up * (0.5**0.5)))
                s.act[f, here, :] = (up * cdf).astype(BF16)
                s.gp[f] = cdf + up * (jnp.exp2(up * up * (-0.5 * LOG2E)) * 0.3989422804014327)
            down = nn(s.act[0, here, :], s.wdown[...]) + nn(s.act[1, here, :], s.wdown_o[...]) + bdown[...]
            n2, rs2 = norm(hidden + down)
            row_mask = (s.kb[whole, 0:1] != 0.0).astype(F32)
            s.output[here, :] = ((n2 * n2g[...] + n2s[...]) * row_mask).astype(BF16)
            cot = s.dout[here, :].astype(F32) * row_mask
            add_small(0, row_sum(cot))
            add_small(1, row_sum(cot * n2))
            d_resid = norm_back(cot * n2g[...], n2, rs2)
            d_down = d_resid.astype(BF16)
            s.ddown[here, :] = d_down
            add_small(2, row_sum(d_down.astype(F32)))
            d_hidden = d_resid
            for f, (w_in, _, w_down, _) in enumerate(halves):
                d_up = (nt(d_down, w_down[...]) * s.gp[f]).astype(BF16)
                s.dup[f, here, :] = d_up
                add_small(3 + f, row_sum(d_up.astype(F32)))
                d_hidden = d_hidden + nt(d_up, w_in[...])
            add_small(5, row_sum(d_hidden))
            add_small(6, row_sum(d_hidden * n1))
            d_pre = norm_back(d_hidden * n1g[...], n1, rs1)
            s.dpre[here, :] = d_pre
            d_attn = d_pre.astype(BF16)
            s.dattn[here, :] = d_attn
            add_small(7, row_sum(d_attn.astype(F32)))
            dm = nt(d_attn, s.wout[...]).astype(BF16)
            do = nt(d_attn, s.wout_o[...]).astype(BF16)
            for h in range(heads):
                s.dmix[h, whole, :] = dm[:, h * HD : (h + 1) * HD]
                s.dmo[h, here, :] = do[:, h * HD : (h + 1) * HD]
            return 0

        lax.fori_loop(0, half // qb, middle, 0)
        dmix_slots = [sems.take() for _ in range(heads)]
        launch(*[across(s.dmo.at[h], s.dmix.at[h, pl.ds(my0, half)], dmix_slots[h]) for h in range(heads)])
        store(s.output, out_h)

        def grad_block(dst, lhs, rhs):
            def body(i, _):
                cols = blk(i * qb, qb)
                dst[cols, :] = tn(lhs[:, cols], rhs[...]).astype(BF16)
                return 0

            lax.fori_loop(0, lhs.shape[1] // qb, body, 0)

        part = {name: across(refs["gs_" + name], refs["gr_" + name]) for name in "abc"}

        def join(name):
            part[name].wait_recv()
            mine, theirs = refs["g_" + name], refs["gr_" + name]
            mine[...] = (mine[...].astype(F32) + theirs[...].astype(F32)).astype(BF16)
            begin(name)

        grad_block(s.gs_a, s.act.at[1], s.ddown)
        launch(part["a"])
        grad_block(s.g_a, s.act.at[0], s.ddown)
        grad_block(s.gs_b, s.hid, s.dup.at[1])
        launch(part["b"])
        join("a")
        grad_block(s.g_b, s.hid, s.dup.at[0])
        theirs = jnp.concatenate([s.mo[h] for h in range(heads)], 1)
        s.gs_c[...] = tn(theirs, s.dattn[...]).astype(BF16)
        launch(part["c"])
        join("b")
        mine = jnp.concatenate([s.mix[h, pl.ds(my0, half), :] for h in range(heads)], 1)
        s.g_c[...] = tn(mine, s.dattn[...]).astype(BF16)
        join("c")

        def turn(i, _):
            rows = blk(i * qb, qb)
            s.xt[:, rows] = s.x[rows, :].T
            for h in range(heads):
                s.kt[h, :, rows] = s.k[h, rows, :].T
            return 0

        lax.fori_loop(0, blocks, turn, 0)
        s.dkacc[...] = jnp.zeros_like(s.dkacc)
        s.dvacc[...] = jnp.zeros_like(s.dvacc)
        for h in range(heads):
            across(s.dmo.at[h], s.dmix.at[h, pl.ds(ot0, half)], dmix_slots[h]).wait_recv()

        def finish_head(h):
            dk = (s.dkacc[h] * (1.0 / LOG2E)).astype(BF16)
            dv = s.dvacc[h].astype(BF16)
            s.dcat[h, :, HD : 2 * HD] = dk
            s.dcat[h, :, 2 * HD :] = dv
            s.sm[8:9, h * HD : (h + 1) * HD] = row_sum(s.dcat[h, :, 0:HD].astype(F32))
            s.sm[8:9, hw + h * HD : hw + (h + 1) * HD] = row_sum(dv.astype(F32))
            dst = s.g_d0 if h == 0 else s.g_d1

            def body(i, _):
                rows = blk(i * 128, 128)
                dst[rows, :] = nn(s.xt[rows, :], s.dcat[h]).astype(BF16)
                return 0

            lax.fori_loop(0, width // 128, body, 0)
            begin("d0" if h == 0 else "d1")

        def advance_all(tokens):
            for token in tokens:
                if token == "head0":
                    finish_head(0)
                else:
                    name, number = token.split(":")
                    advance(name, int(number))

        def attend_back(i, _):
            h = lax.div(i, blocks)
            qi = lax.rem(t * (blocks // 2) + lax.rem(i, blocks), blocks)
            rows = blk(qi * qb, qb)
            d_mixed = s.dmix[h, rows, :].astype(F32) * s.inv[h, rows, :]
            delta = row_sum((d_mixed * s.mix[h, rows, :].astype(F32)).T)
            d_low = d_mixed.astype(BF16)
            weights_t = s.weights[h, qi]
            s.dvacc[h] += nn(weights_t, d_low)
            d_scores = (weights_t.astype(F32) * (nt(s.v[h], d_low) - delta)).astype(BF16)
            s.dkacc[h] += nn(d_scores, s.q[h, rows, :])
            dqt = nn(s.kt[h], d_scores) * (HD ** (-0.5))
            s.dcat[h, rows, 0:HD] = dqt.T.astype(BF16)
            for number, tokens in LOOP.items():

                @pl.when(i == number)
                def _():
                    advance_all(tokens)

            return 0

        lax.fori_loop(0, n_att, attend_back, 0)

        def project_back(i):
            rows = blk(lax.rem(other * (blocks // 2) + i, blocks) * qb, qb)
            wide = jnp.concatenate([s.dcat[h, rows, :] for h in range(heads)], 1)
            wcat = jnp.concatenate(
                [s.wqkv[c][:, h * HD : (h + 1) * HD] for h in range(heads) for c in range(3)], 1
            )
            return nt(wide, wcat)

        def send_rows(i, _):
            s.dxs[blk(i * qb, qb), :] = project_back(i).astype(BF16)
            return 0

        def keep_rows(i, _):
            s.dpre[blk((i - blocks // 2) * qb, qb), :] += project_back(i)
            return 0

        dx_out = across(s.dxs, s.dxr)
        small_t = across(s.sm, s.smt)
        small_groups = ((nx, m1, peer1), (ny, m2, peer2), (nz, zi, peer3))
        small_bufs = ((s.sm0, s.smr1, s.sm1), (s.sm1, s.smr2, s.sm2), (s.sm2, s.smr3, s.sm3))
        small_first = [sems.take(n - 1) for n, _, _ in small_groups]
        assert sems.count == n_sems

        def small_copies(i):
            n, m, peer = small_groups[i]
            src, dst, _ = small_bufs[i]
            return [
                pltpu.make_async_remote_copy(
                    src_ref=src, dst_ref=dst.at[j - 1], send_sem=send_sem.at[small_first[i] + j - 1],
                    recv_sem=recv_sem.at[small_first[i] + j - 1], device_id=peer(lax.rem(m + j, n)), device_id_type=MESH,
                )
                for j in range(1, n)
            ]

        def small_step(number):
            if number == 0:
                launch(small_t)
                return
            if number == 1:
                small_t.wait_recv()
                s.sm0[...] = s.sm[...] + s.smt[...]
                s.sm0[3:4, :] = s.sm[3:4, :] + s.smt[4:5, :]
                s.sm0[8:9, :] = s.sm[8:9, :]
            else:
                src, got, dst = small_bufs[number - 2]
                for c in small_copies(number - 2):
                    c.wait_recv()
                total = src[...]
                for j in range(small_groups[number - 2][0] - 1):
                    total = total + got[j]
                dst[...] = total
            if number <= 3:
                for c in small_copies(number - 1):
                    c.start()
            else:
                small_o[...] = s.sm3[...]

        for token in TAIL:
            if token == "head1":
                finish_head(1)
            elif token == "dx_send":
                lax.fori_loop(0, blocks // 2, send_rows, 0)
                launch(dx_out)
            elif token == "dx_keep":
                lax.fori_loop(blocks // 2, blocks, keep_rows, 0)
            elif token == "dx_end":
                dx_out.wait_recv()
                s.din[...] = (s.dpre[...] + s.dxr[...].astype(F32)).astype(BF16)
                store(s.din, din_h)
            elif token.startswith("sm"):
                small_step(int(token[2:]))
            else:
                advance_all([token])
        for name in red:
            while at[name] <= red[name].last:
                advance(name, at[name])
        for c in all_copies:
            c.wait_send()
        for i in range(3):
            for c in small_copies(i):
                c.wait_send()
        for r in red.values():
            r.drain()
        for c in stores:
            c.wait()

    return kernel, list(scratch.values()), n_sems, n_local, grads


def finish_kernel(grads, half, width, hw):
    def kernel(out_i, din_i, ga, gb, gc, gd0, gd1, small, out_o, din_o, gqkv_o, gout_o, gin_o, gdown_o, bqv_o, *rest):
        rows_o, (v_out, v_din, va, vb, vc, vd0, vd1, fa, fb, fc, fqkv, sems) = rest[:7], rest[7:]
        loads = [
            pltpu.make_async_copy(src, dst, sems.at[i])
            for i, (src, dst) in enumerate(
                ((ga, va), (gb, vb), (gd0, vd0), (gd1, vd1), (gc, vc), (out_i, v_out), (din_i, v_din))
            )
        ]
        stores = [
            pltpu.make_async_copy(src, dst, sems.at[8 + i])
            for i, (src, dst) in enumerate(
                ((fa, gdown_o), (fb, gin_o), (fqkv, gqkv_o), (fc, gout_o), (v_out, out_o), (v_din, din_o))
            )
        ]
        for c in loads:
            c.start()
        for row, ref in zip((7, 6, 5, 3, 2, 1, 0), rows_o):
            ref[...] = small[row : row + 1, :]
        for i in range(2):
            bqv_o[i : i + 1, :] = small[8:9, i * hw : (i + 1) * hw]
        loads[0].wait()
        fa[...] = va[...].astype(F32)
        stores[0].start()
        loads[1].wait()
        fb[...] = vb[...].astype(F32)
        stores[1].start()
        for h, (load, src) in enumerate(((loads[2], vd0), (loads[3], vd1))):
            load.wait()
            for c in range(3):
                fqkv[c, :, h * HD : (h + 1) * HD] = src[:, c * HD : (c + 1) * HD].astype(F32)
        stores[2].start()
        loads[4].wait()
        fc[...] = vc[...].astype(F32)
        stores[3].start()
        loads[5].wait()
        stores[4].start()
        loads[6].wait()
        stores[5].start()
        for c in stores:
            c.wait()

    fh = grads["a"][0]
    shapes = [
        jax.ShapeDtypeStruct((half, width), BF16),
        jax.ShapeDtypeStruct((half, width), BF16),
        jax.ShapeDtypeStruct((3, width, hw), F32),
        jax.ShapeDtypeStruct((hw, width), F32),
        jax.ShapeDtypeStruct((width, fh), F32),
        jax.ShapeDtypeStruct((fh, width), F32),
        jax.ShapeDtypeStruct((2, hw), F32),
        *[jax.ShapeDtypeStruct((1, width), F32)] * 7,
    ]
    any_ = pl.BlockSpec(memory_space=pl.ANY)
    vmem = pl.BlockSpec(memory_space=pltpu.VMEM)
    vm = pltpu.VMEM
    return pl.pallas_call(
        kernel,
        out_shape=shapes,
        in_specs=[any_] * 7 + [vmem],
        out_specs=[any_] * 6 + [vmem] * 8,
        scratch_shapes=[
            vm((half, width), BF16),
            vm((half, width), BF16),
            *[vm(grads[n], BF16) for n in grads],
            *[vm(grads[n], F32) for n in "abc"],
            vm((3, width, hw), F32),
            pltpu.SemaphoreType.DMA((16,)),
        ],
        compiler_params=pltpu.CompilerParams(vmem_limit_bytes=63 * 1024 * 1024),
    )


def solution(mesh):
    chips = mesh.shape["dp"]
    sizes = torus_sizes(chips)

    def on_device(
        inputs, w_qkv, b_qv, w_out, b_out, norm1_gain, norm1_shift, w_in, b_in, w_down, b_down, norm2_gain, norm2_shift,
        segment_ids, d_out,
    ):
        length, width = inputs.shape
        fh = w_in.shape[1]
        hw = w_out.shape[0]
        half = length // 2
        kernel, scratch, n_sems, n_local, grads = make_kernel(sizes, length, width, 2 * fh)
        row = lambda v: v.reshape(1, -1)
        vmem = pl.BlockSpec(memory_space=pltpu.VMEM)
        any_ = pl.BlockSpec(memory_space=pl.ANY)
        shapes = [
            jax.ShapeDtypeStruct((half, width), BF16),
            jax.ShapeDtypeStruct((half, width), BF16),
            *[jax.ShapeDtypeStruct(shape, BF16) for shape in grads.values()],
            jax.ShapeDtypeStruct((16, width), F32),
        ]
        dma = pltpu.SemaphoreType.DMA
        partial_results = pl.pallas_call(
            kernel,
            out_shape=shapes,
            in_specs=[any_, any_, vmem, any_, vmem, vmem, vmem, any_, vmem, any_, vmem, vmem, vmem, vmem, any_],
            out_specs=[any_] * 7 + [vmem],
            scratch_shapes=[*scratch, dma((n_sems,)), dma((n_sems,)), dma((n_local,))],
            compiler_params=pltpu.CompilerParams(
                collective_id=0, has_side_effects=True, vmem_limit_bytes=60 * 1024 * 1024
            ),
        )(
            inputs, w_qkv, b_qv, w_out, row(b_out), row(norm1_gain), row(norm1_shift), w_in, row(b_in), w_down,
            row(b_down), row(norm2_gain), row(norm2_shift), segment_ids, d_out,
        )
        output, d_inputs, g_qkv, g_out, g_in, g_down, g_bqv, *rows = finish_kernel(grads, half, width, hw)(*partial_results)
        g_bout, g_n1g, g_n1s, g_bin, g_bdown, g_n2g, g_n2s = [v.reshape(-1) for v in rows]
        return (
            output, d_inputs, g_qkv, g_bqv, g_out, g_bout, g_n1g, g_n1s, g_in, g_bin, g_down, g_bdown, g_n2g, g_n2s,
        )

    placed = (
        P("dp", None),
        P(None, None, "tensor"),
        P(None, "tensor"),
        P("tensor", None),
        P(),
        P(),
        P(),
        P(None, "tensor"),
        P("tensor"),
        P("tensor", None),
        P(),
        P(),
        P(),
        P("dp", None),
        P(("dp", "tensor"), None),
    )
    return jax.shard_map(
        on_device,
        mesh=mesh,
        in_specs=placed,
        out_specs=(
            P(("dp", "tensor"), None),
            P(("dp", "tensor"), None),
            P(None, None, "tensor"),
            P(None, "tensor"),
            P("tensor", None),
            P(),
            P(),
            P(),
            P(None, "tensor"),
            P("tensor"),
            P("tensor", None),
            P(),
            P(),
            P(),
        ),
        check_vma=False,
    )
```
